8 devices in a mesh: part: 1 (over z), data: 2 (over y), model: 4 (over x, core).
Axes of the slice: x: 2, y: 2, z: 1, core: 2. Of those that a mesh axis runs over, the one named last changes fastest.
Arguments:
- x_seq: bfloat16 [8, 128, 2048], P(('part', 'data'))
- gy_seq: bfloat16 [8, 128, 2048], P(('part', 'data'), None, 'model')
- h_init: float32 [2, 8, 2048], P(None, ('part', 'data'), 'model')
- c_init: float32 [2, 8, 2048], P(None, ('part', 'data'), 'model')
- w_in: bfloat16 [2048, 4, 2048], P(None, None, 'model')
- w_up: bfloat16 [1, 2048, 4, 2048], P(None, None, None, 'model')
- w_rec: bfloat16 [2, 2048, 4, 2048], P(None, None, None, 'model')
- gate_bias: float32 [2, 4, 2048], P(None, None, 'model')
Outputs:
- output 1: bfloat16 [8, 128, 2048], P(('part', 'data'), None, 'model')
- output 2: float32 [2, 8, 2048], P(None, ('part', 'data'), 'model')
- output 3: float32 [2, 8, 2048], P(None, ('part', 'data'), 'model')
- output 4: float32 [2048, 4, 2048], P('part', None, 'model')
- output 5: float32 [1, 2048, 4, 2048], P(None, 'part', None, 'model')
- output 6: float32 [2, 2048, 4, 2048], P(None, 'part', None, 'model')
- output 7: float32 [2, 4, 2048], P(None, 'part', 'model')
All inputs are finite; a program needn't handle non-finite values.
Results may differ from the reference program's by a relative error of at most 0.012509.
Values are sent between devices in bfloat16 or wider.
A program may use at most 1 GiB of HBM per device.

```python
import jax
import jax.numpy as jnp
from jax import lax

BATCH_ROWS = 8
SEQ_LEN = 128
IN_WIDTH = 2048
HIDDEN = 2048
LAYERS = 2


def setup_inputs(seed: int = 0, part: int = 0) -> dict:
    part_key = jax.random.fold_in(jax.random.key(seed), part)
    k_x, k_gy, k_h, k_c = jax.random.split(part_key, 4)
    k_in, k_up, k_rec, k_bias = jax.random.split(jax.random.key(seed + 1), 4)
    rec_scale = 1.5 * HIDDEN ** -0.5
    x_seq = jax.random.normal(k_x, (BATCH_ROWS, SEQ_LEN, IN_WIDTH), jnp.float32)
    gy_seq = jax.random.normal(k_gy, (BATCH_ROWS, SEQ_LEN, HIDDEN), jnp.float32)
    h_init = 0.5 * jax.random.normal(k_h, (LAYERS, BATCH_ROWS, HIDDEN), jnp.float32)
    c_init = jax.random.normal(k_c, (LAYERS, BATCH_ROWS, HIDDEN), jnp.float32)
    w_in = jax.random.normal(k_in, (IN_WIDTH, 4, HIDDEN), jnp.float32) * IN_WIDTH ** -0.5
    w_up = jax.random.normal(k_up, (LAYERS - 1, HIDDEN, 4, HIDDEN), jnp.float32) * rec_scale
    w_rec = jax.random.normal(k_rec, (LAYERS, HIDDEN, 4, HIDDEN), jnp.float32) * rec_scale
    forget_shift = jnp.array([0.0, 1.0, 0.0, 0.0], jnp.float32)[:, None]
    gate_bias = 0.5 * jax.random.normal(k_bias, (LAYERS, 4, HIDDEN), jnp.float32) + forget_shift
    return {
        'x_seq': x_seq.astype(jnp.bfloat16),
        'gy_seq': gy_seq.astype(jnp.bfloat16),
        'h_init': h_init,
        'c_init': c_init,
        'w_in': w_in.astype(jnp.bfloat16),
        'w_up': w_up.astype(jnp.bfloat16),
        'w_rec': w_rec.astype(jnp.bfloat16),
        'gate_bias': gate_bias,
    }


def reference(x_seq, gy_seq, h_init, c_init, w_in, w_up, w_rec, gate_bias):
    inputs = jnp.swapaxes(x_seq.astype(jnp.float32), 0, 1)
    targets = jnp.swapaxes(gy_seq.astype(jnp.float32), 0, 1)
    params = (w_in.astype(jnp.float32), w_up.astype(jnp.float32), w_rec.astype(jnp.float32), gate_bias)

    def as_bf16(values):
        return values + lax.stop_gradient(values.astype(jnp.bfloat16).astype(jnp.float32) - values)

    def stack_loss(weights):
        p_in, p_up, p_rec, p_bias = weights
        layer_seq = inputs
        h_finals = []
        c_finals = []
        for layer_idx in range(LAYERS):
            w_proj = p_in if layer_idx == 0 else p_up[layer_idx - 1]
            w_layer = p_rec[layer_idx]
            pre_gates = jnp.einsum('tbd,dgh->tbgh', layer_seq, w_proj) + p_bias[layer_idx]

            def lstm_step(carry_state, pre_t):
                h_prev, c_prev = carry_state
                gate_pre = pre_t + jnp.einsum('bk,kgh->bgh', as_bf16(h_prev), w_layer)
                sig_gates = jax.nn.sigmoid(gate_pre[:, :3])
                candidate = jnp.tanh(gate_pre[:, 3])
                c_new = sig_gates[:, 1] * c_prev + sig_gates[:, 0] * candidate
                h_new = sig_gates[:, 2] * jnp.tanh(c_new)
                return (h_new, c_new), as_bf16(h_new)

            final_state, layer_seq = lax.scan(lstm_step, (h_init[layer_idx], c_init[layer_idx]), pre_gates)
            h_finals.append(final_state[0])
            c_finals.append(final_state[1])
        loss_val = jnp.sum(layer_seq * targets)
        return loss_val, (layer_seq, jnp.stack(h_finals), jnp.stack(c_finals))

    weight_grads, aux_out = jax.grad(stack_loss, has_aux=True)(params)
    y_seq = jnp.swapaxes(aux_out[0], 0, 1).astype(jnp.bfloat16)
    return (y_seq, aux_out[1], aux_out[2], weight_grads[0], weight_grads[1], weight_grads[2], weight_grads[3])
```

```python
import jax
import jax.numpy as jnp
from jax import lax
from jax.experimental import pallas as pl
from jax.experimental.pallas import tpu as pltpu
from jax.sharding import PartitionSpec as P

MESH = pl.DeviceIdType.MESH
F32 = jnp.float32
BF16 = jnp.bfloat16
CHUNK = 8
PAIRS = CHUNK // 2
ROWS = 4 * CHUNK
VMEM_LIMIT = 60 * 1024 * 1024


def sigm(v):
    return 0.5 * jnp.tanh(0.5 * v) + 0.5


def mm(a, b):
    return jnp.dot(a, b, preferred_element_type=F32)


def place():
    y = lax.axis_index('data')
    m = lax.axis_index('model')
    return y, m, m // 2, m % 2


def dev(y, m):
    return (lax.axis_index('part'), y, m)


def flips(m):
    x = m // 2
    c = m % 2
    return 2 * x + (1 - c), 2 * (1 - x) + c, 2 * (1 - x) + (1 - c)


def remote(src, dst, ssem, rsem, device):
    return pltpu.make_async_remote_copy(src, dst, ssem, rsem, device_id=device, device_id_type=MESH)


def entry_barrier(y, m):
    barrier = pltpu.get_barrier_semaphore()
    for other in flips(m):
        pl.semaphore_signal(barrier, inc=1, device_id=dev(y, other), device_id_type=MESH)
    pl.semaphore_wait(barrier, 3)


def fwd_kernel(wa_hbm, wb_hbm, wup_hbm, prea_hbm, preb_hbm, bias_ref, h0_ref, c0_ref,
               act_hbm, cell_hbm, hist_hbm, hfin_ref, cfin_ref,
               w, wup, prea, preb, actv, cellv, histv, hbuf, hch, cst, hs, hr, pout,
               lsem, osem, xs, xr, hss, hrs, ps, prs):
    y, m, x, c = place()
    beside, across, skew = flips(m)
    nch = hbuf.shape[0]
    hl = hs.shape[3]
    half = 2 * hl
    wide = 4 * hl
    own_cols = pl.ds(pl.multiple_of(c * half, half), half)

    loads = []
    for pos, shard in enumerate((m, across, beside, skew)):
        rows = pl.ds(pl.multiple_of(shard * hl, hl), hl)
        for col, src in enumerate((wa_hbm, wb_hbm)):
            loads.append(pltpu.make_async_copy(
                src.at[rows, :], w.at[pl.ds(pos * hl, hl), pl.ds(col * wide, wide)], lsem.at[len(loads)]))
    for pos, shard in enumerate((0, 2, 1, 3)):
        loads.append(pltpu.make_async_copy(
            wup_hbm.at[pl.ds(shard * hl, hl), :], wup.at[pl.ds(pos * hl, hl), :], lsem.at[len(loads)]))
    for cp in loads:
        cp.start()

    @pl.when(x == 0)
    def _():
        one = pltpu.make_async_copy(prea_hbm, prea, lsem.at[12])
        two = pltpu.make_async_copy(preb_hbm, preb, lsem.at[13])
        one.start()
        two.start()
        one.wait()
        two.wait()

    entry_barrier(y, m)

    def swap(slot, s):
        return remote(hs.at[slot, s], hr.at[slot, s], xs.at[slot, s], xr.at[slot, s], dev(y, beside))

    def hsend(k, dest, i):
        return remote(histv.at[k], hbuf.at[k, :, own_cols], hss.at[i], hrs.at[k, c], dev(y, dest))

    def hrecv(k, core):
        cols = pl.ds(pl.multiple_of(core * half, half), half)
        return remote(histv.at[k], hbuf.at[k, :, cols], hss.at[0], hrs.at[k, core], dev(y, beside))

    def psend(k):
        return remote(pout, preb.at[pl.ds(k * PAIRS, PAIRS)], ps.at[0], prs.at[k], dev(y, across))

    cst[...] = c0_ref[...]
    cellv[0, 0:4, :] = c0_ref[...]
    cellv[0, 4:8, :] = c0_ref[...]
    for s in (0, 1):
        hs[0, s] = h0_ref[:, s * hl:(s + 1) * hl].astype(BF16)
        swap(0, s).start()
    for cp in loads:
        cp.wait()

    def step(k, p, j):
        pair = k * PAIRS + p
        rows = slice(4 * j, 4 * j + 4)
        cols = (slice(0, wide), slice(wide, 2 * wide))
        acc = [mm(hs[j, 0], w[0:hl, cols[s]]) + mm(hs[j, 1], w[hl:half, cols[s]]) for s in (0, 1)]
        swap(j, 0).wait()
        swap(j, 1).wait()
        got = (hr[j, 0], hr[j, 1])
        acc = [acc[s] + (mm(got[0], w[half:half + hl, cols[s]]) + mm(got[1], w[half + hl:, cols[s]])) for s in (0, 1)]
        for s, pre in ((0, prea), (1, preb)):
            base = s * wide
            units = slice(s * hl, (s + 1) * hl)

            def gate(g):
                return acc[s][:, g * hl:(g + 1) * hl] + pre[pair, rows, g * hl:(g + 1) * hl]

            gi = sigm(gate(0))
            gf = sigm(gate(1))
            go = sigm(gate(2))
            gu = jnp.tanh(gate(3))
            cn = gf * cst[:, units] + gi * gu
            hn = go * jnp.tanh(cn)
            hs[1 - j, s] = hn.astype(BF16)
            cst[:, units] = cn
            for g, val in enumerate((gi, gf, go, gu)):
                actv[pair, rows, base + g * hl:base + (g + 1) * hl] = val
            cellv[pair + 1, rows, units] = cn
            hch[p, rows, units] = hn
        swap(1 - j, 0).start()
        swap(1 - j, 1).start()

    def up_product(k):
        return (mm(hbuf[k], wup[...]) + bias_ref[...]).reshape(PAIRS, 8, wide)

    def act_out(k):
        rows = pl.ds(k * PAIRS, PAIRS)
        return pltpu.make_async_copy(actv.at[rows], act_hbm.at[rows], osem.at[0])

    def slot_body(s, _):
        k = s - x
        live = (k >= 0) & (k < nch)

        @pl.when((x == 1) & (s >= 1))
        def _():
            hrecv(k, 0).wait_recv()
            hrecv(k, 1).wait_recv()
            prea[pl.ds(k * PAIRS, PAIRS)] = up_product(k)
            psend(k).wait_recv()

        def pair_body(p, _):
            @pl.when((x == 0) & (s >= 1) & (p == 1))
            def _():
                hrecv(s - 1, 1 - c).wait_recv()

                @pl.when(s >= 2)
                def _():
                    psend(s - 2).wait_send()

                pout[...] = up_product(s - 1)
                psend(s - 1).start()

            @pl.when(live)
            def _():
                step(k, p, 0)
                step(k, p, 1)
            return 0

        lax.fori_loop(0, PAIRS, pair_body, 0)

        @pl.when(live)
        def _():
            block = hch[...].reshape(ROWS, half).astype(BF16)
            histv[k] = block
            act_out(k).start()

            @pl.when(x == 0)
            def _():
                hbuf[k, :, own_cols] = block

                @pl.when(k >= 1)
                def _():
                    for i, dest in enumerate((beside, across, skew)):
                        hsend(k - 1, dest, i).wait_send()
                for i, dest in enumerate((beside, across, skew)):
                    hsend(k, dest, i).start()
        return 0

    lax.fori_loop(0, nch + 1, slot_body, 0)
    swap(0, 0).wait()
    swap(0, 1).wait()
    outs = (pltpu.make_async_copy(histv, hist_hbm, osem.at[1]),
            pltpu.make_async_copy(cellv, cell_hbm, osem.at[2]))
    for cp in outs:
        cp.start()

    @pl.when(x == 0)
    def _():
        for i, dest in enumerate((beside, across, skew)):
            hsend(nch - 1, dest, i).wait_send()
        psend(nch - 1).wait_send()

    hfin_ref[...] = hch[PAIRS - 1, 4:8, :]
    cfin_ref[...] = cst[...]
    for cp in outs:
        cp.wait()
    pltpu.make_async_copy(actv, act_hbm, osem.at[0]).wait()


def bwd_kernel(wta_hbm, wtb_hbm, wupt_hbm, act_hbm, cell_hbm, gy_hbm,
               dg_hbm, dgo_hbm, bias_ref,
               wt, wupt, actv, cellv, dout, dgv, dgr, dgch, dgs, dct, bacc, own, snd, rcv, pin, pout,
               lsem, asem, osem, xs, xr, gs, grs, ps, prs):
    y, m, x, c = place()
    beside, across, skew = flips(m)
    nch = dgv.shape[0]
    half = own.shape[1]
    hl = half // 2
    wide = 4 * hl

    loads = []
    for pos, shard in enumerate((beside, skew, m, across)):
        cols = pl.ds(pl.multiple_of(shard * hl, hl), hl)
        for row, src in enumerate((wta_hbm, wtb_hbm)):
            loads.append(pltpu.make_async_copy(
                src.at[:, cols], wt.at[pl.ds(row * wide, wide), pl.ds(pos * hl, hl)], lsem.at[len(loads)]))
    for pos, shard in enumerate((1 - c, 3 - c, c, 2 + c)):
        cols = pl.ds(pl.multiple_of(shard * hl, hl), hl)
        loads.append(pltpu.make_async_copy(
            wupt_hbm.at[:, cols], wupt.at[:, pl.ds(pos * hl, hl)], lsem.at[len(loads)]))
    loads.append(pltpu.make_async_copy(cell_hbm, cellv, lsem.at[12]))
    for cp in loads:
        cp.start()

    @pl.when(x == 1)
    def _():
        one = pltpu.make_async_copy(gy_hbm, dout, lsem.at[13])
        one.start()
        one.wait()

    def act_in(k):
        rows = pl.ds(k * PAIRS, PAIRS)
        return pltpu.make_async_copy(act_hbm.at[rows], actv.at[rows], asem.at[k])

    def start_act(i, _):
        act_in(nch - 1 - i).start()
        return 0

    lax.fori_loop(0, nch, start_act, 0)
    entry_barrier(y, m)

    def swap(slot):
        return remote(snd.at[slot], rcv.at[slot], xs.at[slot], xr.at[slot], dev(y, beside))

    def gsend(k):
        return remote(dgv.at[k, :, pl.ds(wide, wide)], dgr.at[k], gs.at[0], grs.at[k], dev(y, across))

    def psend(k, pos, dest, src):
        return remote(pout.at[pos], pin.at[src, k], ps.at[pos], prs.at[src, k], dev(y, dest))

    dgs[...] = jnp.zeros(dgs.shape, BF16)
    dct[...] = jnp.zeros(dct.shape, F32)
    bacc[...] = jnp.zeros(bacc.shape, F32)
    for cp in loads:
        cp.wait()

    def step(k, p, j):
        pair = k * PAIRS + p
        rows = slice(4 * j, 4 * j + 4)
        dgl = dgs[...]
        snd[j] = mm(dgl, wt[:, 0:half])
        swap(j).start()
        own[...] = mm(dgl, wt[:, half:])
        swap(j).wait()
        for s in (0, 1):
            base = s * wide
            units = slice(s * hl, (s + 1) * hl)
            gi, gf, go, gu = (actv[pair, rows, base + g * hl:base + (g + 1) * hl] for g in range(4))
            tc = jnp.tanh(cellv[pair + 1, rows, units])
            cp = cellv[pair + 1, 0:4, units] if j else cellv[pair, 4:8, units]
            dh = dout[pair, rows, units] + own[:, units] + rcv[j, :, units]
            dc = dct[:, units] + dh * go * (1.0 - tc * tc)
            dct[:, units] = dc * gf
            grads = (dc * gu * gi * (1.0 - gi), dc * cp * gf * (1.0 - gf),
                     dh * tc * go * (1.0 - go), dc * gi * (1.0 - gu * gu))
            for g, val in enumerate(grads):
                cols = slice(base + g * hl, base + (g + 1) * hl)
                bacc[:, cols] += val
                dgs[:, cols] = val.astype(BF16)
                dgch[p, rows, cols] = val

    def slot_body(s, _):
        k = nch - 1 - s + (1 - x)
        live = (k >= 0) & (k < nch)

        @pl.when(live)
        def _():
            act_in(k).wait()

        @pl.when((x == 0) & live)
        def _():
            gsend(k).wait_recv()
            block = dgr[k]

            @pl.when(s >= 2)
            def _():
                psend(k + 1, 0, beside, 2).wait_send()
            pout[0] = mm(block, wupt[:, 0:half]).reshape(PAIRS, 8, half)
            psend(k, 0, beside, 2).start()
            part = mm(block, wupt[:, half:]).reshape(PAIRS, 8, half)
            for src in (0, 1, 2):
                psend(k, 0, beside, src).wait_recv()
            dout[pl.ds(k * PAIRS, PAIRS)] = part + pin[0, k] + pin[1, k] + pin[2, k]

        @pl.when(live)
        def _():
            def pair_body(i, _):
                step(k, PAIRS - 1 - i, 1)
                step(k, PAIRS - 1 - i, 0)
                return 0

            lax.fori_loop(0, PAIRS, pair_body, 0)
            dgv[k] = dgch[...].reshape(ROWS, 2 * wide).astype(BF16)

        @pl.when((x == 1) & live)
        def _():
            @pl.when(s >= 1)
            def _():
                gsend(k + 1).wait_send()
                psend(k + 1, 0, skew, c).wait_send()
                psend(k + 1, 1, across, c).wait_send()
            gsend(k).start()
            block = dgv[k, :, 0:wide]
            pout[0] = mm(block, wupt[:, 0:half]).reshape(PAIRS, 8, half)
            psend(k, 0, skew, c).start()
            pout[1] = mm(block, wupt[:, half:]).reshape(PAIRS, 8, half)
            psend(k, 1, across, c).start()
        return 0

    lax.fori_loop(0, nch + 1, slot_body, 0)
    outs = (pltpu.make_async_copy(dgv, dg_hbm, osem.at[0]),
            pltpu.make_async_copy(dgr, dgo_hbm, osem.at[1]))
    for cp in outs:
        cp.start()
    bias_ref[...] = bacc[...]

    @pl.when(x == 0)
    def _():
        psend(0, 0, beside, 2).wait_send()

    @pl.when(x == 1)
    def _():
        gsend(0).wait_send()
        psend(0, 0, skew, c).wait_send()
        psend(0, 1, across, c).wait_send()
    for cp in outs:
        cp.wait()


def any_spec():
    return pl.BlockSpec(memory_space=pl.ANY)


def vmem_spec():
    return pl.BlockSpec(memory_space=pltpu.VMEM)


def sds(shape, dtype):
    return jax.ShapeDtypeStruct(shape, dtype)


def run_fwd(wa, wb, wup, prea, preb, bias, h0, c0):
    hidden, wide = wa.shape
    hl = wide // 4
    half = 2 * hl
    npair = prea.shape[0]
    nch = npair // PAIRS
    dma = pltpu.SemaphoreType.DMA
    return pl.pallas_call(
        fwd_kernel,
        name='lstm_forward',
        out_shape=(sds((npair, 8, 2 * wide), F32), sds((npair + 1, 8, half), F32),
                   sds((nch, ROWS, half), BF16), sds((4, half), F32), sds((4, half), F32)),
        in_specs=[any_spec()] * 5 + [vmem_spec()] * 3,
        out_specs=(any_spec(), any_spec(), any_spec(), vmem_spec(), vmem_spec()),
        scratch_shapes=[
            pltpu.VMEM((hidden, 2 * wide), BF16), pltpu.VMEM((hidden, wide), BF16),
            pltpu.VMEM((npair, 8, wide), F32), pltpu.VMEM((npair, 8, wide), F32),
            pltpu.VMEM((npair, 8, 2 * wide), F32), pltpu.VMEM((npair + 1, 8, half), F32),
            pltpu.VMEM((nch, ROWS, half), BF16), pltpu.VMEM((nch, ROWS, hidden), BF16),
            pltpu.VMEM((PAIRS, 8, half), F32), pltpu.VMEM((4, half), F32),
            pltpu.VMEM((2, 2, 4, hl), BF16), pltpu.VMEM((2, 2, 4, hl), BF16),
            pltpu.VMEM((PAIRS, 8, wide), F32),
            dma((14,)), dma((3,)), dma((2, 2)), dma((2, 2)), dma((3,)), dma((nch, 2)), dma((1,)), dma((nch,)),
        ],
        compiler_params=pltpu.CompilerParams(collective_id=0, has_side_effects=True, vmem_limit_bytes=VMEM_LIMIT),
    )(wa, wb, wup, prea, preb, bias, h0, c0)


def run_bwd(wta, wtb, wupt, act, cell, gy):
    wide, hidden = wta.shape
    hl = wide // 4
    half = 2 * hl
    npair = act.shape[0]
    nch = npair // PAIRS
    dma = pltpu.SemaphoreType.DMA
    return pl.pallas_call(
        bwd_kernel,
        name='lstm_backward',
        out_shape=(sds((nch, ROWS, 2 * wide), BF16), sds((nch, ROWS, wide), BF16), sds((4, 2 * wide), F32)),
        in_specs=[any_spec()] * 6,
        out_specs=(any_spec(), any_spec(), vmem_spec()),
        scratch_shapes=[
            pltpu.VMEM((2 * wide, hidden), BF16), pltpu.VMEM((wide, hidden), BF16),
            pltpu.VMEM((npair, 8, 2 * wide), F32), pltpu.VMEM((npair + 1, 8, half), F32),
            pltpu.VMEM((npair, 8, half), F32),
            pltpu.VMEM((nch, ROWS, 2 * wide), BF16), pltpu.VMEM((nch, ROWS, wide), BF16),
            pltpu.VMEM((PAIRS, 8, 2 * wide), F32), pltpu.VMEM((4, 2 * wide), BF16),
            pltpu.VMEM((4, half), F32), pltpu.VMEM((4, 2 * wide), F32),
            pltpu.VMEM((4, half), F32), pltpu.VMEM((2, 4, half), F32), pltpu.VMEM((2, 4, half), F32),
            pltpu.VMEM((3, nch, PAIRS, 8, half), F32), pltpu.VMEM((2, PAIRS, 8, half), F32),
            dma((14,)), dma((nch,)), dma((2,)), dma((2,)), dma((2,)), dma((1,)), dma((nch,)), dma((2,)), dma((3, nch)),
        ],
        compiler_params=pltpu.CompilerParams(collective_id=1, has_side_effects=True, vmem_limit_bytes=VMEM_LIMIT),
    )(wta, wtb, wupt, act, cell, gy)


ACROSS = [(0, 2), (1, 3), (2, 0), (3, 1)]


def solution(mesh):
    batch_axes = ('part', 'data')
    seq_spec = P(batch_axes, None, 'model')
    state_spec = P(None, batch_axes, 'model')
    weight_spec = P(None, None, None, 'model')
    in_specs = (P(batch_axes, None, None), seq_spec, state_spec, state_spec,
                P(None, None, 'model'), weight_spec, weight_spec, P(None, None, 'model'))
    out_specs = (seq_spec, state_spec, state_spec, P('part', None, 'model'),
                 P(None, 'part', None, 'model'), P(None, 'part', None, 'model'), P(None, 'part', 'model'))

    def local_program(x_seq, gy_seq, h_init, c_init, w_in, w_up, w_rec, gate_bias):
        rows, seq_len, width = x_seq.shape
        hl = w_in.shape[2]
        wide = 4 * hl
        half = 2 * hl
        hidden = w_rec.shape[1]
        npair = seq_len // 2
        nch = seq_len // CHUNK
        m = lax.axis_index('model')
        x = m // 2

        def across(v):
            return lax.ppermute(v, 'model', ACROSS)

        def pick(v, i):
            return lax.dynamic_index_in_dim(v, i, 0, keepdims=False)

        wa = pick(w_rec, x)
        wb = across(pick(w_rec, 1 - x))
        wa = wa.reshape(hidden, wide)
        wb = wb.reshape(hidden, wide)
        wup = w_up[0].reshape(hidden, wide)
        xt = jnp.swapaxes(x_seq, 0, 1).reshape(seq_len * rows, width)
        pre = mm(xt, w_in.reshape(width, wide)) + gate_bias[0].reshape(1, wide)
        pre = pre.reshape(npair, 8, wide)
        preb = across(pre)
        h0 = jnp.concatenate([pick(h_init, x), across(pick(h_init, 1 - x))], axis=1)
        c0 = jnp.concatenate([pick(c_init, x), across(pick(c_init, 1 - x))], axis=1)
        act, cell, hist, hfin, cfin = run_fwd(wa, wb, wup, pre, preb, gate_bias[1].reshape(1, wide), h0, c0)

        gy = jnp.concatenate([gy_seq, across(gy_seq)], axis=2)
        gy = jnp.swapaxes(gy, 0, 1).reshape(npair, 8, half).astype(F32)
        dg, dg_up, bias_part = run_bwd(wa.T, wb.T, wup.T, act, cell, gy)

        every = lax.all_gather(hist.reshape(seq_len * 4, half), ('data', 'model'))
        every = every.reshape(2, 4, seq_len, 4, 2, hl)

        def layer_hist(layer):
            a = every[:, 2 * layer:2 * layer + 2]
            first, second = a[..., layer, :], a[..., 1 - layer, :]
            full = jnp.stack([first, second], axis=1)
            return jnp.moveaxis(full.reshape(2, 4, seq_len, 4, hl), 1, 3).reshape(2, seq_len, 4, hidden)

        h_low = layer_hist(0)
        h_top = layer_hist(1)
        init_all = lax.all_gather(h_init.astype(BF16), 'model', axis=2, tiled=True)
        init_all = lax.all_gather(init_all, 'data')

        def shifted(full, layer):
            return jnp.concatenate([init_all[:, layer][:, None], full[:, :-1]], axis=1)

        x_all = lax.all_gather(jnp.swapaxes(x_seq, 0, 1), 'data')
        dg = dg.reshape(seq_len * 4, 2 * wide)
        mine = lax.all_gather(dg[:, :wide], 'data')
        other = lax.all_gather(across(dg[:, wide:]), 'data')
        dg_low = jnp.where(x == 0, mine, other).reshape(-1, wide)
        dg_top = jnp.where(x == 0, other, mine).reshape(-1, wide)

        def outer(a, b):
            return jnp.einsum('rk,rn->kn', a.reshape(-1, a.shape[-1]), b, preferred_element_type=F32)

        dw_in = outer(x_all, dg_low).reshape(width, 4, hl)
        dw_up = outer(h_low, dg_top).reshape(1, hidden, 4, hl)
        dw_rec = jnp.stack([outer(shifted(h_low, 0), dg_low), outer(shifted(h_top, 1), dg_top)])
        dw_rec = dw_rec.reshape(2, hidden, 4, hl)

        bsum = jnp.sum(bias_part, axis=0)
        b_mine = bsum[:wide]
        b_other = across(bsum[wide:])
        bias = jnp.where(x == 0, jnp.stack([b_mine, b_other]), jnp.stack([b_other, b_mine]))
        bias = lax.psum(bias, 'data').reshape(2, 4, hl)

        def both(v):
            mine, other = v[:, :hl], across(v[:, hl:])
            return jnp.where(x == 0, jnp.stack([mine, other]), jnp.stack([other, mine]))

        own_top = lax.dynamic_slice_in_dim(lax.dynamic_index_in_dim(h_top, lax.axis_index('data'), 0, keepdims=False),
                                           m * hl, hl, axis=2)
        y_local = jnp.swapaxes(own_top, 0, 1)
        return (y_local, both(hfin), both(cfin), dw_in, dw_up, dw_rec, bias)

    return jax.shard_map(local_program, mesh=mesh, in_specs=in_specs, out_specs=out_specs, check_vma=False)
```

```python
import jax
import jax.numpy as jnp
from jax import lax
from jax.experimental import pallas as pl
from jax.experimental.pallas import tpu as pltpu
from jax.sharding import PartitionSpec as P

MESH = pl.DeviceIdType.MESH
F32 = jnp.float32
BF16 = jnp.bfloat16
LANES = 128
BATCH = 4
CHUNK = 8
PAIRS = CHUNK // 2
ROWS = BATCH * CHUNK
KB = 128
NX = 8
VMEM_LIMIT = 63 * 1024 * 1024


def sigm(v):
    return 0.5 * jnp.tanh(0.5 * v) + 0.5


def mm(a, b):
    return jnp.dot(a, b, preferred_element_type=F32)


def place():
    y = lax.axis_index('data')
    m = lax.axis_index('model')
    return y, m, m // 2, m % 2


def dev(y, m):
    return (lax.axis_index('part'), y, m)


def flips(m):
    x = m // 2
    c = m % 2
    return 2 * x + (1 - c), 2 * (1 - x) + c, 2 * (1 - x) + (1 - c)


def everyone(y, m):
    beside, across, skew = flips(m)
    return ((y, beside), (y, across), (y, skew), (1 - y, m), (1 - y, beside), (1 - y, across), (1 - y, skew))


def remote(src, dst, ssem, rsem, device):
    return pltpu.make_async_remote_copy(src, dst, ssem, rsem, device_id=device, device_id_type=MESH)


def local(src, dst, sem):
    return pltpu.make_async_copy(src, dst, sem)


def entry_barrier(y, m):
    barrier = pltpu.get_barrier_semaphore()
    for oy, om in everyone(y, m):
        pl.semaphore_signal(barrier, inc=1, device_id=dev(oy, om), device_id_type=MESH)
    pl.semaphore_wait(barrier, 7)


def aligned(i, n):
    return pl.ds(pl.multiple_of(i * n, n), n)


def gate_row(bias_ref, layer):
    return jnp.concatenate([bias_ref[layer, g:g + 1, :] for g in range(4)], axis=1)


def prep_kernel(wrec_hbm, wup_hbm, win_hbm, x_hbm, gy_hbm, hc_ref, bias_ref,
                wa_hbm, wb_hbm, wat_hbm, wbt_hbm, wup2_hbm, wupt_hbm, pre_hbm, xt_hbm, gyt_hbm, hcb_ref, init_ref,
                rin, rup, ra, rb, spread, wst, wtst, win, xin, xf, xb, prev, gyin, gyb, ib, initv, hcv,
                lsem, osem, jsem, ssx, rsx, ssy, rsy, sss, rss, gsem):
    y, m, x, c = place()
    beside, across, skew = flips(m)
    hl = hc_ref.shape[3]
    per = hl // LANES
    stride = 4 * per
    span = KB * stride
    seq = xin.shape[1]
    whole = rb.shape[0]
    part_rows = whole // 2

    loads = [local(x_hbm, xin, lsem.at[0]),
             local(win_hbm, rin, lsem.at[1]),
             local(wrec_hbm.at[aligned(x, whole), :], ra, lsem.at[2]),
             local(wup_hbm, rup, lsem.at[3]),
             local(gy_hbm, gyin, lsem.at[4])]
    for cp in loads:
        cp.start()
    entry_barrier(y, m)

    def xsend(i):
        off = y * part_rows + i * span
        src = wrec_hbm.at[pl.ds(pl.multiple_of((1 - x) * whole + off, span), span), :]
        return remote(src, rb.at[pl.ds(pl.multiple_of(off, span), span), :], ssx.at[i], rsx.at[i], dev(y, across))

    def ysend(i):
        rows = pl.ds(pl.multiple_of(y * part_rows + i * span, span), span)
        return remote(rb.at[rows, :], rb.at[rows, :], ssy.at[i], rsy.at[i], dev(1 - y, m))

    def small(i, dest_y, dest_m):
        slot = 0 if i < 3 else 1
        dst = initv.at[:, slot, :, pl.ds(pl.multiple_of(c * 2 * hl + x * hl, hl), hl)]
        return remote(ib, dst, sss.at[i], rss.at[i], dev(dest_y, dest_m))

    def state_send():
        return remote(hc_ref.at[1 - x], hcv, sss.at[7], rss.at[7], dev(y, across))

    ib[...] = hc_ref[:, 0].astype(BF16)
    initv[:, 0, :, pl.ds(pl.multiple_of(c * 2 * hl + x * hl, hl), hl)] = ib[...]
    for i, (oy, om) in enumerate(everyone(y, m)):
        small(i, oy, om).start()
    state_send().start()
    for i in range(NX):
        xsend(i).start()

    loads[0].wait()
    for t in range(xb.shape[1] // LANES):
        cols = slice(t * LANES, (t + 1) * LANES)
        for b in range(BATCH):
            xf[t % 4, pl.ds(b, seq, stride=BATCH), :] = xin[b, :, cols].astype(F32)
        xb[:, cols] = xf[t % 4].astype(BF16)
    xout = local(xb, xt_hbm, osem.at[0])
    xout.start()
    loads[4].wait()
    for t in range(per):
        cols = slice(t * LANES, (t + 1) * LANES)
        for b in range(BATCH):
            xf[t % 4, pl.ds(b, seq, stride=BATCH), :] = gyin[b, :, cols].astype(F32)
        gyb[:, cols] = xf[t % 4].astype(BF16)
    gout = local(gyb, gyt_hbm.at[0], osem.at[1])
    gout.start()

    def gy_send():
        return remote(gyb, gyt_hbm.at[1], gsem.at[0], gsem.at[1], dev(y, across))

    @pl.when(x == 0)
    def _():
        gy_send().start()

    for cp in loads[1:4]:
        cp.wait()

    def tiles(buf, raw, blk):
        spread[buf] = raw[aligned(blk, span), :].astype(F32)
        for g in range(4):
            for ct in range(per):
                yield g * hl + ct * LANES, spread[buf, pl.ds(ct * 4 + g, KB, stride=stride), :]

    def job_out(pos, blk, wo, wto):
        return (local(wst.at[pos], wo.at[aligned(blk, KB), :], jsem.at[pos, 0]),
                local(wtst.at[pos], wto.at[:, aligned(blk, KB)], jsem.at[pos, 1]))

    def job(pos, raw, blk, wo, wto):
        for off, tile in tiles(pos % 2, raw, blk):
            wst[pos, :, off:off + LANES] = tile.astype(BF16)
            wtst[pos, off:off + LANES, :] = tile.T.astype(BF16)
        for cp in job_out(pos, blk, wo, wto):
            cp.start()

    def job_wait(pos, wo, wto):
        for cp in job_out(pos, 0, wo, wto):
            cp.wait()

    early = NX // 2

    def body(i, _):
        @pl.when(i < early)
        def _():
            for q in range(4):
                blk = i * 4 + q
                for off, tile in tiles(q % 2, rin, blk):
                    win[aligned(blk, KB), off:off + LANES] = tile.astype(BF16)

        @pl.when(i == early)
        def _():
            row = gate_row(bias_ref, 0)
            nr = KB

            def pre_body(r, _):
                val = mm(xb[aligned(r, nr), :], win[...]) + row
                prev[aligned(r, nr // 8)] = val.reshape(nr // 8, 8, val.shape[1])
                return 0

            lax.fori_loop(0, xb.shape[0] // nr, pre_body, 0)
            local(prev, pre_hbm, osem.at[2]).start()

        @pl.when(i >= early)
        def _():
            for q in range(4):
                if q < 2:
                    @pl.when(i > early)
                    def _():
                        job_wait(q, wup2_hbm, wupt_hbm)
                else:
                    job_wait(q % 2, wup2_hbm, wupt_hbm)
                job(q % 2, rup, (i - early) * 4 + q, wup2_hbm, wupt_hbm)

        for q in range(2):
            @pl.when(i > 0)
            def _():
                job_wait(2 + q, wa_hbm, wat_hbm)
            job(2 + q, ra, i * 2 + q, wa_hbm, wat_hbm)

        xsend(i).wait_recv()
        ysend(i).start()

        @pl.when(i > 0)
        def _():
            job_wait(4, wb_hbm, wbt_hbm)
        job(4, rb, y * NX + i, wb_hbm, wbt_hbm)

        @pl.when(i > 0)
        def _():
            ysend(i - 1).wait_recv()

            @pl.when(i > 1)
            def _():
                job_wait(5, wb_hbm, wbt_hbm)
            job(5, rb, (1 - y) * NX + i - 1, wb_hbm, wbt_hbm)
        return 0

    lax.fori_loop(0, NX, body, 0)
    job_wait(5, wb_hbm, wbt_hbm)
    ysend(NX - 1).wait_recv()
    job(5, rb, (1 - y) * NX + NX - 1, wb_hbm, wbt_hbm)

    for i, (oy, om) in enumerate(everyone(y, m)):
        small(i, oy, om).wait()
    state_send().wait()
    hcb_ref[...] = hcv[...]
    init_ref[...] = initv[...]

    @pl.when(x == 0)
    def _():
        gy_send().wait_send()

    @pl.when(x == 1)
    def _():
        gy_send().wait_recv()

    for i in range(NX):
        xsend(i).wait_send()
        ysend(i).wait_send()
    for q in range(2):
        job_wait(q, wup2_hbm, wupt_hbm)
        job_wait(2 + q, wa_hbm, wat_hbm)
    job_wait(4, wb_hbm, wbt_hbm)
    job_wait(5, wb_hbm, wbt_hbm)
    xout.wait()
    gout.wait()
    local(prev, pre_hbm, osem.at[2]).wait()


def fwd_kernel(wa_hbm, wb_hbm, wup_hbm, pre_hbm, xt_hbm, hc_ref, hcb_ref, bias_ref,
               act_hbm, cell_hbm, lown_hbm, loth_hbm, town_hbm, toth_hbm, xoth_hbm, hfin_ref, cfin_ref,
               w, wup, prea, preb, actv, cellv, histv, hbuf, hch, cst, hs, hr, pout, fin, finr,
               lsem, psem, osem, xs, xr, hss, hrs, ps, prs, csem, fsem):
    y, m, x, c = place()
    beside, across, skew = flips(m)
    nch = hbuf.shape[0]
    hl = hs.shape[3]
    half = 2 * hl
    wide = 4 * hl
    own_cols = pl.ds(pl.multiple_of(c * half, half), half)
    others = everyone(y, m)

    loads = []
    for pos, shard in enumerate((m, across, beside, skew)):
        for col, src in enumerate((wa_hbm, wb_hbm)):
            loads.append(local(src.at[aligned(shard, hl), :], w.at[pl.ds(pos * hl, hl), pl.ds(col * wide, wide)],
                               lsem.at[len(loads)]))
    up_loads = [local(wup_hbm.at[pl.ds(shard * hl, hl), :], wup.at[pl.ds(pos * hl, hl), :], lsem.at[8 + pos])
                for pos, shard in enumerate((0, 2, 1, 3))]
    for cp in loads:
        cp.start()

    def pre_load(k):
        rows = pl.ds(k * PAIRS, PAIRS)
        return local(pre_hbm.at[rows], prea.at[rows], psem.at[k])

    @pl.when(x == 0)
    def _():
        def start(k, _):
            pre_load(k).start()
            return 0
        lax.fori_loop(0, nch, start, 0)

    for cp in up_loads:
        cp.start()

    entry_barrier(y, m)

    def swap(slot, s):
        return remote(hs.at[slot, s], hr.at[slot, s], xs.at[slot, s], xr.at[slot, s], dev(y, beside))

    def pre_send(k):
        rows = pl.ds(k * PAIRS, PAIRS)
        return remote(pre_hbm.at[rows], preb.at[rows], ps.at[k], prs.at[k], dev(y, across))

    def up_send(k):
        return remote(pout, preb.at[pl.ds(k * PAIRS, PAIRS)], ps.at[k], prs.at[k], dev(y, across))

    def x_send():
        return remote(xt_hbm, xoth_hbm, fsem.at[2], fsem.at[3], dev(1 - y, m))

    @pl.when(x == 1)
    def _():
        def start(k, _):
            pre_send(k).start()
            return 0
        lax.fori_loop(0, nch, start, 0)

    x_send().start()

    def low_send(k, i):
        oy, om = others[i]
        if i < 3:
            return remote(histv.at[k], hbuf.at[k, :, own_cols], hss.at[i], hrs.at[k, c], dev(oy, om))
        return remote(histv.at[k], loth_hbm.at[aligned(k, ROWS), own_cols], hss.at[i], csem.at[0], dev(oy, om))

    def top_send(k, i):
        oy, om = others[i]
        dst, sem = (town_hbm, csem.at[1]) if i < 3 else (toth_hbm, csem.at[2])
        return remote(histv.at[k], dst.at[aligned(k, ROWS), own_cols], hss.at[i], sem, dev(oy, om))

    def hrecv(k, core):
        cols = pl.ds(pl.multiple_of(core * half, half), half)
        return remote(histv.at[k], hbuf.at[k, :, cols], hss.at[0], hrs.at[k, core], dev(y, beside))

    def own_top(k):
        return local(histv.at[k], town_hbm.at[aligned(k, ROWS), own_cols], osem.at[3])

    init = [jnp.where(x == 0, hc_ref[0], hc_ref[1]), hcb_ref[...]]
    for s in (0, 1):
        units = slice(s * hl, (s + 1) * hl)
        hs[0, s] = init[s][0].astype(BF16)
        cst[:, units] = init[s][1]
        cellv[0, 0:4, units] = init[s][1]
        cellv[0, 4:8, units] = init[s][1]
        swap(0, s).start()
    for cp in loads:
        cp.wait()
    for cp in up_loads:
        cp.wait()

    def step(k, p, j):
        pair = k * PAIRS + p
        rows = slice(4 * j, 4 * j + 4)
        cols = (slice(0, wide), slice(wide, 2 * wide))
        acc = [mm(hs[j, 0], w[0:hl, cols[s]]) + mm(hs[j, 1], w[hl:half, cols[s]]) for s in (0, 1)]
        swap(j, 0).wait()
        swap(j, 1).wait()
        got = (hr[j, 0], hr[j, 1])
        acc = [acc[s] + (mm(got[0], w[half:half + hl, cols[s]]) + mm(got[1], w[half + hl:, cols[s]])) for s in (0, 1)]
        for s, pre in ((0, prea), (1, preb)):
            base = s * wide
            units = slice(s * hl, (s + 1) * hl)

            def gate(g):
                return acc[s][:, g * hl:(g + 1) * hl] + pre[pair, rows, g * hl:(g + 1) * hl]

            gi = sigm(gate(0))
            gf = sigm(gate(1))
            go = sigm(gate(2))
            gu = jnp.tanh(gate(3))
            cn = gf * cst[:, units] + gi * gu
            hn = go * jnp.tanh(cn)
            hs[1 - j, s] = hn.astype(BF16)
            cst[:, units] = cn
            for g, val in enumerate((gi, gf, go, gu)):
                actv[pair, rows, base + g * hl:base + (g + 1) * hl] = val
            cellv[pair + 1, rows, units] = cn
            hch[p, rows, units] = hn
        swap(1 - j, 0).start()
        swap(1 - j, 1).start()

    def up_product(k):
        return (mm(hbuf[k], wup[...]) + gate_row(bias_ref, 1)).reshape(PAIRS, 8, wide)

    def act_out(k):
        rows = pl.ds(k * PAIRS, PAIRS)
        return local(actv.at[rows], act_hbm.at[rows], osem.at[0])

    def slot_body(s, _):
        k = s - x
        live = (k >= 0) & (k < nch)

        @pl.when((x == 1) & live)
        def _():
            hrecv(k, 0).wait_recv()
            hrecv(k, 1).wait_recv()
            prea[pl.ds(k * PAIRS, PAIRS)] = up_product(k)

        @pl.when((x == 0) & live)
        def _():
            pre_load(k).wait()

        @pl.when(live)
        def _():
            up_send(k).wait_recv()

        def pair_body(p, _):
            @pl.when((x == 0) & (s >= 1) & (p == 1))
            def _():
                hrecv(s - 1, 1 - c).wait_recv()

                @pl.when(s >= 2)
                def _():
                    up_send(s - 2).wait_send()

                pout[...] = up_product(s - 1)
                up_send(s - 1).start()

            @pl.when(live)
            def _():
                step(k, p, 0)
                step(k, p, 1)
            return 0

        lax.fori_loop(0, PAIRS, pair_body, 0)

        @pl.when(live)
        def _():
            act_out(k).start()

            @pl.when(x == 0)
            def _():
                block = hch[...].reshape(ROWS, half).astype(BF16)
                histv[k] = block
                hbuf[k, :, own_cols] = block

                @pl.when(k >= 1)
                def _():
                    for i in range(7):
                        low_send(k - 1, i).wait_send()
                for i in range(7):
                    low_send(k, i).start()

            @pl.when(x == 1)
            def _():
                block = hch[...].reshape(ROWS, half).astype(BF16)
                histv[k, :, 0:hl] = block[:, hl:half]
                histv[k, :, hl:half] = block[:, 0:hl]

                @pl.when(k >= 1)
                def _():
                    for i in range(7):
                        top_send(k - 1, i).wait_send()
                for i in range(7):
                    top_send(k, i).start()
                own_top(k).start()
        return 0

    lax.fori_loop(0, nch + 1, slot_body, 0)
    swap(0, 0).wait()
    swap(0, 1).wait()

    def fin_send():
        return remote(fin, finr, fsem.at[0], fsem.at[1], dev(y, across))

    fin[0] = hch[PAIRS - 1, 4:8, hl:half]
    fin[1] = cst[:, hl:half]
    fin_send().start()
    local(cellv, cell_hbm, osem.at[2]).start()

    @pl.when(x == 0)
    def _():
        for i in range(7):
            low_send(nch - 1, i).wait_send()
        up_send(nch - 1).wait_send()
        local(town_hbm, town_hbm, csem.at[1]).wait()

    @pl.when(x == 1)
    def _():
        for i in range(7):
            top_send(nch - 1, i).wait_send()

        def drain(k, _):
            pre_send(k).wait_send()
            return 0
        lax.fori_loop(0, nch, drain, 0)
        part = town_hbm.at[:, pl.ds(0, half)]
        local(part, part, csem.at[1]).wait()
        local(part, part, osem.at[3]).wait()

    def low_out(k):
        return local(hbuf.at[k], lown_hbm.at[aligned(k, ROWS), :], osem.at[1])

    def low_start(k, _):
        low_out(k).start()
        return 0

    lax.fori_loop(0, nch, low_start, 0)
    local(loth_hbm, loth_hbm, csem.at[0]).wait()
    local(toth_hbm, toth_hbm, csem.at[2]).wait()
    x_send().wait()
    fin_send().wait()
    mine = [hch[PAIRS - 1, 4:8, 0:hl], cst[:, 0:hl]]
    for ref, i in ((hfin_ref, 0), (cfin_ref, 1)):
        ref[0] = jnp.where(x == 0, mine[i], finr[i])
        ref[1] = jnp.where(x == 0, finr[i], mine[i])
    local(lown_hbm, lown_hbm, osem.at[1]).wait()
    local(cellv, cell_hbm, osem.at[2]).wait()
    local(actv, act_hbm, osem.at[0]).wait()


def bwd_kernel(wta_hbm, wtb_hbm, wupt_hbm, act_hbm, cell_hbm, gy_hbm,
               dg_hbm, bias_ref,
               wt, wupt, actv, cellv, dout, gyv, dgv, dgr, dgch, dgs, dct, bacc, own, snd, rcv, pin, pout, bsnd, brcv,
               lsem, asem, osem, xs, xr, gs, grs, ps, prs, csem, bsem):
    y, m, x, c = place()
    beside, across, skew = flips(m)
    nch = dgv.shape[0]
    half = own.shape[1]
    hl = half // 2
    wide = 4 * hl

    loads = []
    for pos, shard in enumerate((beside, skew, m, across)):
        for row, src in enumerate((wta_hbm, wtb_hbm)):
            loads.append(local(src.at[:, aligned(shard, hl)], wt.at[pl.ds(row * wide, wide), pl.ds(pos * hl, hl)],
                               lsem.at[len(loads)]))
    for pos, shard in enumerate((1 - c, 3 - c, c, 2 + c)):
        loads.append(local(wupt_hbm.at[:, aligned(shard, hl)], wupt.at[:, pl.ds(pos * hl, hl)], lsem.at[len(loads)]))
    loads.append(local(cell_hbm, cellv, lsem.at[12]))
    for cp in loads:
        cp.start()

    @pl.when(x == 1)
    def _():
        cp = local(gy_hbm, gyv, lsem.at[13])
        cp.start()
        cp.wait()
        for s in (0, 1):
            dout[:, :, s * hl:(s + 1) * hl] = gyv[s].astype(F32).reshape(nch * PAIRS, 8, hl)

    def act_in(k):
        rows = pl.ds(k * PAIRS, PAIRS)
        return local(act_hbm.at[rows], actv.at[rows], asem.at[k])

    def start_act(i, _):
        act_in(nch - 1 - i).start()
        return 0

    lax.fori_loop(0, nch, start_act, 0)
    entry_barrier(y, m)

    def swap(slot):
        return remote(snd.at[slot], rcv.at[slot], xs.at[slot], xr.at[slot], dev(y, beside))

    part_a = pl.ds(0, wide)
    part_b = pl.ds(wide, wide)

    def up_grads(k):
        return remote(dgv.at[k, :, part_b], dgr.at[k], gs.at[0], grs.at[k], dev(y, across))

    def sends(k, top):
        rows = aligned(k, ROWS)
        layer = 1 if top else 0
        mine = remote(dgv.at[k, :, part_a], dg_hbm.at[layer, 1, rows, :], gs.at[1], csem.at[0], dev(1 - y, m))
        far = remote(dgv.at[k, :, part_b], dg_hbm.at[layer, 1, rows, :], gs.at[2], csem.at[1], dev(1 - y, across))
        near = up_grads(k) if top else remote(
            dgv.at[k, :, part_b], dg_hbm.at[0, 0, rows, :], gs.at[0], csem.at[2], dev(y, across))
        return near, mine, far

    def keep(k, top):
        return local(dgv.at[k, :, part_a], dg_hbm.at[1 if top else 0, 0, aligned(k, ROWS), :], osem.at[0])

    def keep_up(k):
        return local(dgr.at[k], dg_hbm.at[1, 0, aligned(k, ROWS), :], osem.at[1])

    def psend(k, pos, dest, src):
        return remote(pout.at[pos], pin.at[src, k], ps.at[pos], prs.at[src, k], dev(y, dest))

    dgs[...] = jnp.zeros(dgs.shape, BF16)
    dct[...] = jnp.zeros(dct.shape, F32)
    bacc[...] = jnp.zeros(bacc.shape, F32)
    for cp in loads:
        cp.wait()

    def step(k, p, j):
        pair = k * PAIRS + p
        rows = slice(4 * j, 4 * j + 4)
        dgl = dgs[...]
        snd[j] = mm(dgl, wt[:, 0:half])
        swap(j).start()
        own[...] = mm(dgl, wt[:, half:])
        swap(j).wait()
        for s in (0, 1):
            base = s * wide
            units = slice(s * hl, (s + 1) * hl)
            gi, gf, go, gu = (actv[pair, rows, base + g * hl:base + (g + 1) * hl] for g in range(4))
            tc = jnp.tanh(cellv[pair + 1, rows, units])
            cp = cellv[pair + 1, 0:4, units] if j else cellv[pair, 4:8, units]
            dh = dout[pair, rows, units] + own[:, units] + rcv[j, :, units]
            dc = dct[:, units] + dh * go * (1.0 - tc * tc)
            dct[:, units] = dc * gf
            grads = (dc * gu * gi * (1.0 - gi), dc * cp * gf * (1.0 - gf),
                     dh * tc * go * (1.0 - go), dc * gi * (1.0 - gu * gu))
            for g, val in enumerate(grads):
                cols = slice(base + g * hl, base + (g + 1) * hl)
                bacc[:, cols] += val
                dgs[:, cols] = val.astype(BF16)
                dgch[p, rows, cols] = val

    def slot_body(s, _):
        k = nch - 1 - s + (1 - x)
        live = (k >= 0) & (k < nch)

        @pl.when(live)
        def _():
            act_in(k).wait()

        @pl.when((x == 0) & live)
        def _():
            up_grads(k).wait_recv()
            keep_up(k).start()
            block = dgr[k]

            @pl.when(s >= 2)
            def _():
                psend(k + 1, 0, beside, 2).wait_send()
            pout[0] = mm(block, wupt[:, 0:half]).reshape(PAIRS, 8, half)
            psend(k, 0, beside, 2).start()
            part = mm(block, wupt[:, half:]).reshape(PAIRS, 8, half)
            for src in (0, 1, 2):
                psend(k, 0, beside, src).wait_recv()
            dout[pl.ds(k * PAIRS, PAIRS)] = part + pin[0, k] + pin[1, k] + pin[2, k]

        @pl.when(live)
        def _():
            def pair_body(i, _):
                step(k, PAIRS - 1 - i, 1)
                step(k, PAIRS - 1 - i, 0)
                return 0

            lax.fori_loop(0, PAIRS, pair_body, 0)
            dgv[k] = dgch[...].reshape(ROWS, 2 * wide).astype(BF16)

        @pl.when((x == 0) & live)
        def _():
            @pl.when(s >= 2)
            def _():
                for cp in sends(k + 1, False):
                    cp.wait_send()
            for cp in sends(k, False):
                cp.start()
            keep(k, False).start()

        @pl.when((x == 1) & live)
        def _():
            @pl.when(s >= 1)
            def _():
                for cp in sends(k + 1, True):
                    cp.wait_send()
                psend(k + 1, 0, skew, c).wait_send()
                psend(k + 1, 1, across, c).wait_send()
            for cp in sends(k, True):
                cp.start()
            keep(k, True).start()
            block = dgv[k, :, 0:wide]
            pout[0] = mm(block, wupt[:, 0:half]).reshape(PAIRS, 8, half)
            psend(k, 0, skew, c).start()
            pout[1] = mm(block, wupt[:, half:]).reshape(PAIRS, 8, half)
            psend(k, 1, across, c).start()
        return 0

    lax.fori_loop(0, nch + 1, slot_body, 0)

    bsnd[0] = bacc[:, 0:wide]
    bsnd[1] = bacc[:, wide:]
    shares = (remote(bsnd.at[0], brcv.at[0], bsem.at[0], bsem.at[3], dev(1 - y, m)),
              remote(bsnd.at[1], brcv.at[1], bsem.at[1], bsem.at[4], dev(y, across)),
              remote(bsnd.at[1], brcv.at[2], bsem.at[2], bsem.at[5], dev(1 - y, across)))
    for cp in shares:
        cp.start()

    quarter = dg_hbm.at[0, 0]

    @pl.when(x == 0)
    def _():
        psend(0, 0, beside, 2).wait_send()
        for cp in sends(0, False):
            cp.wait_send()
        local(quarter, quarter, osem.at[1]).wait()

    @pl.when(x == 1)
    def _():
        for cp in sends(0, True):
            cp.wait_send()
        psend(0, 0, skew, c).wait_send()
        psend(0, 1, across, c).wait_send()
        local(quarter, quarter, csem.at[2]).wait()

    local(quarter, quarter, csem.at[0]).wait()
    local(quarter, quarter, csem.at[1]).wait()
    local(quarter, quarter, osem.at[0]).wait()
    for cp in shares:
        cp.wait()
    same = jnp.sum(bsnd[0] + brcv[0], axis=0, keepdims=True)
    cross = jnp.sum(brcv[1] + brcv[2], axis=0, keepdims=True)
    low = jnp.where(x == 0, same, cross)
    top = jnp.where(x == 0, cross, same)
    for g in range(4):
        bias_ref[0, g:g + 1, :] = low[:, g * hl:(g + 1) * hl]
        bias_ref[1, g:g + 1, :] = top[:, g * hl:(g + 1) * hl]


def grad_kernel(xo_hbm, xf_hbm, lo_hbm, lf_hbm, to_hbm, tf_hbm, init_ref, dg_hbm,
                dwin_hbm, dwup_hbm, dwrec_hbm, y_ref,
                xv, hlow, htop, dlow, dtop, shf, yf, stage, lsem, osem):
    hidden = hlow.shape[1]
    srows = lo_hbm.shape[0]
    kb = 256
    hl = hidden // 4
    wide = dlow.shape[1]
    nblk = hidden // kb
    per = hl // LANES
    raw = kb * 4 * per
    nq = hl // kb
    m = lax.axis_index('model')
    x = m // 2
    c = m % 2
    lo = pl.ds(0, srows)
    hi = pl.ds(srows, srows)
    srcs = ((xo_hbm, xv.at[lo, :]), (xf_hbm, xv.at[hi, :]), (dg_hbm.at[0, 0], dlow.at[lo, :]), (dg_hbm.at[0, 1], dlow.at[hi, :]),
            (lo_hbm, hlow.at[lo, :]), (lf_hbm, hlow.at[hi, :]), (dg_hbm.at[1, 0], dtop.at[lo, :]), (dg_hbm.at[1, 1], dtop.at[hi, :]),
            (to_hbm, htop.at[lo, :]), (tf_hbm, htop.at[hi, :]))
    loads = [local(a, b, lsem.at[i]) for i, (a, b) in enumerate(srcs)]
    for cp in loads:
        cp.start()

    def core_row(i):
        q = i // nq
        return ((q % 2) * 2 + q // 2) * nq + i % nq

    def out_copy(slot, dst, off):
        return local(stage.at[slot], dst.at[aligned(off, raw), :], osem.at[slot])

    def emit(count, lhs, grads, dst, off):
        slot = lax.rem(count, 2)

        @pl.when(count >= 2)
        def _():
            out_copy(slot, dst, off).wait()
        res = mm(lhs.T, grads[...])
        for g in range(4):
            for ct in range(per):
                col = g * hl + ct * LANES
                stage[slot, pl.ds(ct * 4 + g, kb, stride=4 * per), :] = res[:, col:col + LANES]
        out_copy(slot, dst, off).start()

    def shifted(h, layer, cols):
        for part in (0, 1):
            base = part * srows
            shf[base + 4:base + srows, :] = h[pl.ds(base, srows), cols].astype(F32)[:srows - 4]
            shf[base:base + 4, :] = init_ref[layer, part, :, cols].astype(F32)
        return shf[...].astype(BF16)

    for cp in loads[0:4]:
        cp.wait()

    def phase0(i, _):
        emit(i, xv[:, aligned(i, kb)], dlow, dwin_hbm, i)
        return 0

    def phase1(i, _):
        emit(i + nblk, shifted(hlow, 0, aligned(i, kb)), dlow, dwrec_hbm, core_row(i))
        return 0

    def phase2(i, _):
        emit(i + 2 * nblk, hlow[:, aligned(i, kb)], dtop, dwup_hbm, core_row(i))
        return 0

    def phase3(i, _):
        emit(i + 3 * nblk, shifted(htop, 1, aligned(i, kb)), dtop, dwrec_hbm, nblk + core_row(i))
        return 0

    lax.fori_loop(0, nblk, phase0, 0)
    for cp in loads[4:6]:
        cp.wait()
    lax.fori_loop(0, nblk, phase1, 0)
    for cp in loads[6:8]:
        cp.wait()
    lax.fori_loop(0, nblk, phase2, 0)
    for cp in loads[8:10]:
        cp.wait()
    for t in range(per):
        yf[t] = htop[0:srows, pl.ds(pl.multiple_of(c * 2 * hl + x * hl + t * LANES, LANES), LANES)].astype(F32)
        for b in range(BATCH):
            y_ref[b, :, t * LANES:(t + 1) * LANES] = yf[t, pl.ds(b, srows // BATCH, stride=BATCH), :].astype(BF16)
    lax.fori_loop(0, nblk, phase3, 0)
    for slot in (0, 1):
        out_copy(slot, dwrec_hbm, 0).wait()


def any_spec():
    return pl.BlockSpec(memory_space=pl.ANY)


def vmem_spec():
    return pl.BlockSpec(memory_space=pltpu.VMEM)


def sds(shape, dtype):
    return jax.ShapeDtypeStruct(shape, dtype)


DMA = pltpu.SemaphoreType.DMA


def comm_params(i):
    return pltpu.CompilerParams(collective_id=i, has_side_effects=True, vmem_limit_bytes=VMEM_LIMIT)


def run_prep(wrec, wup, win, x, gy, hc, bias):
    batch, seq, width = x.shape
    hl = gy.shape[2]
    wide = 4 * hl
    hidden = 4 * hl
    rows = batch * seq
    raw = win.shape[0]
    per = hl // LANES
    span = KB * 4 * per
    square = sds((hidden, wide), BF16)
    vm = pltpu.VMEM
    return pl.pallas_call(
        prep_kernel,
        name='lstm_prepare',
        out_shape=(square,) * 6 + (sds((rows // 8, 8, wide), F32), sds((rows, width), BF16), sds((2, rows, hl), BF16),
                                   sds((2, 4, hl), F32), sds((2, 2, 4, hidden), BF16)),
        in_specs=[any_spec()] * 5 + [vmem_spec()] * 2,
        out_specs=(any_spec(),) * 9 + (vmem_spec(),) * 2,
        scratch_shapes=[
            vm((raw, LANES), BF16), vm((raw, LANES), BF16), vm((raw, LANES), BF16), vm((raw, LANES), BF16),
            vm((2, span, LANES), F32), vm((6, KB, wide), BF16), vm((6, wide, KB), BF16), vm((width, wide), BF16),
            vm(x.shape, BF16), vm((4, rows, LANES), F32), vm((rows, width), BF16), vm((rows // 8, 8, wide), F32),
            vm(gy.shape, BF16), vm((rows, hl), BF16), vm((2, 4, hl), BF16),
            vm((2, 2, 4, hidden), BF16), vm((2, 4, hl), F32),
            DMA((5,)), DMA((3,)), DMA((6, 2)), DMA((NX,)), DMA((NX,)), DMA((NX,)), DMA((NX,)), DMA((8,)), DMA((8,)), DMA((2,)),
        ],
        compiler_params=comm_params(0),
    )(wrec, wup, win, x, gy, hc, bias)


def run_fwd(wa, wb, wup, pre, xt, hc, hcb, bias):
    hidden, wide = wa.shape
    hl = wide // 4
    half = 2 * hl
    npair = pre.shape[0]
    nch = npair // PAIRS
    rows = npair * 8
    hist = sds((rows, hidden), BF16)
    vm = pltpu.VMEM
    return pl.pallas_call(
        fwd_kernel,
        name='lstm_forward',
        out_shape=(sds((npair, 8, 2 * wide), F32), sds((npair + 1, 8, half), F32), hist, hist, hist, hist,
                   sds(xt.shape, BF16), sds((2, 4, hl), F32), sds((2, 4, hl), F32)),
        in_specs=[any_spec()] * 5 + [vmem_spec()] * 3,
        out_specs=(any_spec(),) * 7 + (vmem_spec(),) * 2,
        scratch_shapes=[
            vm((hidden, 2 * wide), BF16), vm((hidden, wide), BF16),
            vm((npair, 8, wide), F32), vm((npair, 8, wide), F32),
            vm((npair, 8, 2 * wide), F32), vm((npair + 1, 8, half), F32),
            vm((nch, ROWS, half), BF16), vm((nch, ROWS, hidden), BF16),
            vm((PAIRS, 8, half), F32), vm((4, half), F32),
            vm((2, 2, 4, hl), BF16), vm((2, 2, 4, hl), BF16),
            vm((PAIRS, 8, wide), F32), vm((2, 4, hl), F32), vm((2, 4, hl), F32),
            DMA((12,)), DMA((nch,)), DMA((4,)), DMA((2, 2)), DMA((2, 2)), DMA((7,)), DMA((nch, 2)),
            DMA((nch,)), DMA((nch,)), DMA((3,)), DMA((4,)),
        ],
        compiler_params=comm_params(1),
    )(wa, wb, wup, pre, xt, hc, hcb, bias)


def run_bwd(wta, wtb, wupt, act, cell, gy):
    wide, hidden = wta.shape
    hl = wide // 4
    half = 2 * hl
    npair = act.shape[0]
    nch = npair // PAIRS
    rows = npair * 8
    vm = pltpu.VMEM
    return pl.pallas_call(
        bwd_kernel,
        name='lstm_backward',
        out_shape=(sds((2, 2, rows, wide), BF16), sds((2, 4, hl), F32)),
        in_specs=[any_spec()] * 6,
        out_specs=(any_spec(), vmem_spec()),
        scratch_shapes=[
            vm((2 * wide, hidden), BF16), vm((wide, hidden), BF16),
            vm((npair, 8, 2 * wide), F32), vm((npair + 1, 8, half), F32),
            vm((npair, 8, half), F32), vm((2, rows, hl), BF16),
            vm((nch, ROWS, 2 * wide), BF16), vm((nch, ROWS, wide), BF16),
            vm((PAIRS, 8, 2 * wide), F32), vm((4, 2 * wide), BF16),
            vm((4, half), F32), vm((4, 2 * wide), F32),
            vm((4, half), F32), vm((2, 4, half), F32), vm((2, 4, half), F32),
            vm((3, nch, PAIRS, 8, half), F32), vm((2, PAIRS, 8, half), F32),
            vm((2, 4, wide), F32), vm((3, 4, wide), F32),
            DMA((14,)), DMA((nch,)), DMA((2,)), DMA((2,)), DMA((2,)), DMA((3,)), DMA((nch,)), DMA((2,)), DMA((3, nch)),
            DMA((3,)), DMA((6,)),
        ],
        compiler_params=comm_params(2),
    )(wta, wtb, wupt, act, cell, gy)


def run_grads(xo, xf, lo, lf, to, tf, init, dg):
    srows, hidden = lo.shape
    rows = 2 * srows
    wide = dg.shape[3]
    raw = hidden * wide // LANES
    hl = wide // 4
    kb = 256
    vm = pltpu.VMEM
    return pl.pallas_call(
        grad_kernel,
        name='weight_grads',
        out_shape=(sds((raw, LANES), F32), sds((raw, LANES), F32), sds((2 * raw, LANES), F32),
                   sds((BATCH, srows // BATCH, hl), BF16)),
        in_specs=[any_spec()] * 6 + [vmem_spec(), any_spec()],
        out_specs=(any_spec(),) * 3 + (vmem_spec(),),
        scratch_shapes=[vm((rows, hidden), BF16)] * 3 + [vm((rows, wide), BF16)] * 2 + [
            vm((rows, kb), F32), vm((hl // LANES, srows, LANES), F32), vm((2, kb * wide // LANES, LANES), F32), DMA((10,)), DMA((2,))],
        compiler_params=pltpu.CompilerParams(vmem_limit_bytes=VMEM_LIMIT),
    )(xo, xf, lo, lf, to, tf, init, dg)


def to_raw(w):
    hl = w.shape[-1]
    w = w.reshape(-1, 4, hl // LANES, LANES)
    return jnp.swapaxes(w, 1, 2).reshape(-1, LANES)


def from_raw(v, lead, hl):
    v = v.reshape(-1, hl // LANES, 4, LANES)
    return jnp.swapaxes(v, 1, 2).reshape(lead + (-1, 4, hl))


def solution(mesh):
    batch_axes = ('part', 'data')
    seq_spec = P(batch_axes, None, 'model')
    state_spec = P(None, batch_axes, 'model')
    weight_spec = P(None, None, None, 'model')
    in_specs = (P(batch_axes, None, None), seq_spec, state_spec, state_spec,
                P(None, None, 'model'), weight_spec, weight_spec, P(None, None, 'model'))
    out_specs = (seq_spec, state_spec, state_spec, P('part', None, 'model'),
                 P(None, 'part', None, 'model'), P(None, 'part', None, 'model'), P(None, 'part', 'model'))

    def local_program(x_seq, gy_seq, h_init, c_init, w_in, w_up, w_rec, gate_bias):
        hl = w_in.shape[2]
        hc = jnp.stack([h_init, c_init], axis=1)
        wa, wb, wat, wbt, wup, wupt, pre, xt, gyt, hcb, init = run_prep(
            to_raw(w_rec), to_raw(w_up), to_raw(w_in), x_seq, gy_seq, hc, gate_bias)
        act, cell, low_own, low_far, top_own, top_far, x_far, h_last, c_last = run_fwd(
            wa, wb, wup, pre, xt, hc, hcb, gate_bias)
        dg, bias = run_bwd(wat, wbt, wupt, act, cell, gyt)
        dw_in, dw_up, dw_rec, y_out = run_grads(xt, x_far, low_own, low_far, top_own, top_far, init, dg)
        return (y_out, h_last, c_last, from_raw(dw_in, (), hl), from_raw(dw_up, (1,), hl),
                from_raw(dw_rec, (2,), hl), bias)

    return jax.shard_map(local_program, mesh=mesh, in_specs=in_specs, out_specs=out_specs, check_vma=False)
```

```python
import jax
import jax.numpy as jnp
from jax import lax
from jax.experimental import pallas as pl
from jax.experimental.pallas import tpu as pltpu
from jax.sharding import PartitionSpec as P

MESH = pl.DeviceIdType.MESH
F32 = jnp.float32
BF16 = jnp.bfloat16
LANES = 128
BATCH = 4
CHUNK = 8
_0, _1, _2 = range(3)
BOTH = (_0, _1)
GATES = range(4)
PAIRS = CHUNK // _2
ROWS = BATCH * CHUNK
KB = 128
NX = 8
VMEM_LIMIT = 63 * 1024 * 1024


def sigm(v):
    return 0.5 * jnp.tanh(0.5 * v) + 0.5


def mm(a, b):
    return jnp.dot(a, b, preferred_element_type=F32)


def place():
    y = lax.axis_index('data')
    m = lax.axis_index('model')
    return y, m, m // _2, m % _2


def dev(y, m):
    return (lax.axis_index('part'), y, m)


def flips(m):
    x = m // _2
    c = m % _2
    return _2 * x + (_1 - c), _2 * (_1 - x) + c, _2 * (_1 - x) + (_1 - c)


def everyone(y, m):
    beside, across, skew = flips(m)
    return ((y, beside), (y, across), (y, skew), (_1 - y, m), (_1 - y, beside), (_1 - y, across), (_1 - y, skew))


def remote(src, dst, ssem, rsem, device):
    return pltpu.make_async_remote_copy(src, dst, ssem, rsem, device_id=device, device_id_type=MESH)


def local(src, dst, sem):
    return pltpu.make_async_copy(src, dst, sem)


def entry_barrier(y, m):
    barrier = pltpu.get_barrier_semaphore()
    for oy, om in everyone(y, m):
        pl.semaphore_signal(barrier, inc=_1, device_id=dev(oy, om), device_id_type=MESH)
    pl.semaphore_wait(barrier, 7)


def part(i, n, base=_0):
    return slice(base + i * n, base + (i + _1) * n)


def aligned(i, n):
    return pl.ds(pl.multiple_of(i * n, n), n)


def gate_row(bias_ref, layer):
    return jnp.concatenate([bias_ref[layer, g:g + _1, :] for g in GATES], axis=_1)


def prep_kernel(wrec_hbm, wup_hbm, win_hbm, x_hbm, gy_hbm, hc_ref, bias_ref,
                wa_hbm, wb_hbm, wat_hbm, wbt_hbm, wup2_hbm, wupt_hbm, pre_hbm, xt_hbm, gyt_hbm, hcb_ref, init_ref,
                rin, rup, ra, rb, spread, wst, wtst, win, xin, xf, xb, prev, gyin, gyb, ib, initv, hcv,
                lsem, osem, jsem, ssx, rsx, ssy, rsy, sss, rss, gsem):
    y, m, x, c = place()
    beside, across, skew = flips(m)
    hl = hc_ref.shape[3]
    per = hl // LANES
    stride = 4 * per
    span = KB * stride
    seq = xin.shape[_1]
    whole = rb.shape[_0]
    part_rows = whole // _2

    loads = [local(x_hbm, xin, lsem.at[_0]),
             local(win_hbm, rin, lsem.at[_1]),
             local(wrec_hbm.at[aligned(x, whole), :], ra, lsem.at[_2]),
             local(wup_hbm, rup, lsem.at[3]),
             local(gy_hbm, gyin, lsem.at[4])]
    for cp in loads:
        cp.start()
    entry_barrier(y, m)

    def xsend(i):
        off = y * part_rows + i * span
        src = wrec_hbm.at[pl.ds(pl.multiple_of((_1 - x) * whole + off, span), span), :]
        return remote(src, rb.at[pl.ds(pl.multiple_of(off, span), span), :], ssx.at[i], rsx.at[i], dev(y, across))

    def ysend(i):
        rows = pl.ds(pl.multiple_of(y * part_rows + i * span, span), span)
        return remote(rb.at[rows, :], rb.at[rows, :], ssy.at[i], rsy.at[i], dev(_1 - y, m))

    def small(i, dest_y, dest_m):
        slot = _0 if i < 3 else _1
        dst = initv.at[:, slot, :, pl.ds(pl.multiple_of(c * _2 * hl + x * hl, hl), hl)]
        return remote(ib, dst, sss.at[i], rss.at[i], dev(dest_y, dest_m))

    def state_send():
        return remote(hc_ref.at[_1 - x], hcv, sss.at[7], rss.at[7], dev(y, across))

    ib[...] = hc_ref[:, _0].astype(BF16)
    initv[:, _0, :, pl.ds(pl.multiple_of(c * _2 * hl + x * hl, hl), hl)] = ib[...]
    for i, (oy, om) in enumerate(everyone(y, m)):
        small(i, oy, om).start()
    state_send().start()
    for i in range(NX):
        xsend(i).start()

    loads[_0].wait()
    for t in range(xb.shape[_1] // LANES):
        cols = part(t, LANES)
        for b in range(BATCH):
            xf[t % 4, pl.ds(b, seq, stride=BATCH), :] = xin[b, :, cols].astype(F32)
        xb[:, cols] = xf[t % 4].astype(BF16)
    xout = local(xb, xt_hbm, osem.at[_0])
    xout.start()
    loads[4].wait()
    for t in range(per):
        cols = part(t, LANES)
        for b in range(BATCH):
            xf[t % 4, pl.ds(b, seq, stride=BATCH), :] = gyin[b, :, cols].astype(F32)
        gyb[:, cols] = xf[t % 4].astype(BF16)
    gout = local(gyb, gyt_hbm.at[_0], osem.at[_1])
    gout.start()

    def gy_send():
        return remote(gyb, gyt_hbm.at[_1], gsem.at[_0], gsem.at[_1], dev(y, across))

    @pl.when(x == _0)
    def _():
        gy_send().start()

    for cp in loads[_1:4]:
        cp.wait()

    def tiles(buf, raw, blk):
        spread[buf] = raw[aligned(blk, span), :].astype(F32)
        for g in GATES:
            for ct in range(per):
                yield g * hl + ct * LANES, spread[buf, pl.ds(ct * 4 + g, KB, stride=stride), :]

    def job_out(pos, blk, wo, wto):
        return (local(wst.at[pos], wo.at[aligned(blk, KB), :], jsem.at[pos, _0]),
                local(wtst.at[pos], wto.at[:, aligned(blk, KB)], jsem.at[pos, _1]))

    def job(pos, raw, blk, wo, wto):
        for off, tile in tiles(pos % _2, raw, blk):
            wst[pos, :, off:off + LANES] = tile.astype(BF16)
            wtst[pos, off:off + LANES, :] = tile.T.astype(BF16)
        for cp in job_out(pos, blk, wo, wto):
            cp.start()

    def job_wait(pos, wo, wto):
        for cp in job_out(pos, _0, wo, wto):
            cp.wait()

    early = NX // _2

    def body(i, _):
        @pl.when(i < early)
        def _():
            for q in range(4):
                blk = i * 4 + q
                for off, tile in tiles(q % _2, rin, blk):
                    win[aligned(blk, KB), off:off + LANES] = tile.astype(BF16)

        @pl.when(i == early)
        def _():
            row = gate_row(bias_ref, _0)
            nr = KB

            def pre_body(r, _):
                val = mm(xb[aligned(r, nr), :], win[...]) + row
                prev[aligned(r, nr // 8)] = val.reshape(nr // 8, 8, val.shape[_1])
                return _0

            lax.fori_loop(_0, xb.shape[_0] // nr, pre_body, _0)
            local(prev, pre_hbm, osem.at[_2]).start()

        @pl.when(i >= early)
        def _():
            for q in range(4):
                if q < _2:
                    @pl.when(i > early)
                    def _():
                        job_wait(q, wup2_hbm, wupt_hbm)
                else:
                    job_wait(q % _2, wup2_hbm, wupt_hbm)
                job(q % _2, rup, (i - early) * 4 + q, wup2_hbm, wupt_hbm)

        for q in range(_2):
            @pl.when(i > _0)
            def _():
                job_wait(_2 + q, wa_hbm, wat_hbm)
            job(_2 + q, ra, i * _2 + q, wa_hbm, wat_hbm)

        xsend(i).wait_recv()
        ysend(i).start()

        @pl.when(i > _0)
        def _():
            job_wait(4, wb_hbm, wbt_hbm)
        job(4, rb, y * NX + i, wb_hbm, wbt_hbm)

        @pl.when(i > _0)
        def _():
            ysend(i - _1).wait_recv()

            @pl.when(i > _1)
            def _():
                job_wait(5, wb_hbm, wbt_hbm)
            job(5, rb, (_1 - y) * NX + i - _1, wb_hbm, wbt_hbm)
        return _0

    lax.fori_loop(_0, NX, body, _0)
    job_wait(5, wb_hbm, wbt_hbm)
    ysend(NX - _1).wait_recv()
    job(5, rb, (_1 - y) * NX + NX - _1, wb_hbm, wbt_hbm)

    for i, (oy, om) in enumerate(everyone(y, m)):
        small(i, oy, om).wait()
    state_send().wait()
    hcb_ref[...] = hcv[...]
    init_ref[...] = initv[...]

    @pl.when(x == _0)
    def _():
        gy_send().wait_send()

    @pl.when(x == _1)
    def _():
        gy_send().wait_recv()

    for i in range(NX):
        xsend(i).wait_send()
        ysend(i).wait_send()
    for q in range(_2):
        job_wait(q, wup2_hbm, wupt_hbm)
        job_wait(_2 + q, wa_hbm, wat_hbm)
    job_wait(4, wb_hbm, wbt_hbm)
    job_wait(5, wb_hbm, wbt_hbm)
    xout.wait()
    gout.wait()
    local(prev, pre_hbm, osem.at[_2]).wait()


def fwd_kernel(wa_hbm, wb_hbm, wup_hbm, pre_hbm, xt_hbm, hc_ref, hcb_ref, bias_ref,
               act_hbm, cell_hbm, lown_hbm, loth_hbm, town_hbm, toth_hbm, xoth_hbm, last_ref, fin_ref,
               w, wup, prea, preb, actv, cellv, histv, hbuf, hch, cst, hs, hr,
               lsem, psem, osem, xs, xr, hss, hrs, ps, prs, csem, fsem):
    y, m, x, c = place()
    beside, across, skew = flips(m)
    nch = hbuf.shape[_0]
    npair = nch * PAIRS
    hl = hs.shape[3]
    half = _2 * hl
    wide = 4 * hl
    own_cols = pl.ds(pl.multiple_of(c * half, half), half)
    others = everyone(y, m)

    loads = []
    for pos, shard in enumerate((m, across, beside, skew)):
        for col, src in enumerate((wa_hbm, wb_hbm)):
            loads.append(local(src.at[aligned(shard, hl), :], w.at[pl.ds(pos * hl, hl), pl.ds(col * wide, wide)],
                               lsem.at[len(loads)]))
    up_loads = [local(wup_hbm.at[pl.ds(shard * hl, hl), :], wup.at[pl.ds(pos * hl, hl), :], lsem.at[8 + pos])
                for pos, shard in enumerate((_0, _2, _1, 3))]
    for cp in loads:
        cp.start()

    def pre_load(k):
        rows = pl.ds(k * PAIRS, PAIRS)
        return local(pre_hbm.at[rows], prea.at[rows], psem.at[k])

    @pl.when(x == _0)
    def _():
        def start(k, _):
            pre_load(k).start()
            return _0
        lax.fori_loop(_0, nch, start, _0)

    for cp in up_loads:
        cp.start()

    entry_barrier(y, m)

    def swap(slot, s):
        return remote(hs.at[slot, s], hr.at[slot, s], xs.at[slot, s], xr.at[slot, s], dev(y, beside))

    def pre_send(i):
        return remote(pre_hbm.at[i], preb.at[i], fsem.at[_0], prs.at[i], dev(y, across))

    def up_send(k, p):
        return remote(prea.at[npair + p], preb.at[k * PAIRS + p], ps.at[p], prs.at[k * PAIRS + p], dev(y, across))

    def x_send():
        return remote(xt_hbm, xoth_hbm, fsem.at[_1], fsem.at[_2], dev(_1 - y, m))

    @pl.when(x == _1)
    def _():
        def start(i, _):
            pre_send(i).start()
            return _0
        lax.fori_loop(_0, npair, start, _0)

    x_send().start()

    def low_send(k, i):
        oy, om = others[i]
        if i < 3:
            return remote(histv.at[k], hbuf.at[k, :, own_cols], hss.at[i], hrs.at[k, c], dev(oy, om))
        return remote(histv.at[k], loth_hbm.at[aligned(k, ROWS), own_cols], hss.at[i], csem.at[_0], dev(oy, om))

    def top_send(k, i):
        oy, om = others[i]
        dst, sem = (town_hbm, csem.at[_1]) if i < 3 else (toth_hbm, csem.at[_2])
        return remote(histv.at[k], dst.at[aligned(k, ROWS), own_cols], hss.at[i], sem, dev(oy, om))

    def hrecv(k, core):
        cols = pl.ds(pl.multiple_of(core * half, half), half)
        return remote(histv.at[k], hbuf.at[k, :, cols], hss.at[_0], hrs.at[k, core], dev(y, beside))

    def own_top(k):
        return local(histv.at[k], town_hbm.at[aligned(k, ROWS), own_cols], osem.at[3])

    init = [jnp.where(x == _0, hc_ref[_0], hc_ref[_1]), hcb_ref[...]]
    for s in BOTH:
        units = part(s, hl)
        hs[_0, s] = init[s][_0].astype(BF16)
        cst[:, units] = init[s][_1]
        cellv[_0, _0:4, units] = init[s][_1]
        cellv[_0, 4:8, units] = init[s][_1]
        swap(_0, s).start()
    for cp in loads:
        cp.wait()
    for cp in up_loads:
        cp.wait()

    def step(k, p, j, between):
        pair = k * PAIRS + p
        rows = part(j, BATCH)
        cols = (slice(_0, wide), slice(wide, _2 * wide))
        acc = [mm(hs[j, _0], w[_0:hl, cols[s]]) + mm(hs[j, _1], w[hl:half, cols[s]]) for s in BOTH]
        swap(j, _0).wait()
        swap(j, _1).wait()
        between()
        got = (hr[j, _0], hr[j, _1])
        acc = [acc[s] + (mm(got[_0], w[half:half + hl, cols[s]]) + mm(got[_1], w[half + hl:, cols[s]])) for s in BOTH]
        for s, pre in ((_0, prea), (_1, preb)):
            base = s * wide
            units = part(s, hl)

            def gate(g):
                return acc[s][:, part(g, hl)] + pre[pair, rows, part(g, hl)]

            gi = sigm(gate(_0))
            gf = sigm(gate(_1))
            go = sigm(gate(_2))
            gu = jnp.tanh(gate(3))
            cn = gf * cst[:, units] + gi * gu
            hn = go * jnp.tanh(cn)
            hs[_1 - j, s] = hn.astype(BF16)
            cst[:, units] = cn
            for g, val in enumerate((gi, gf, go, gu)):
                actv[pair, rows, part(g, hl, base)] = val
            cellv[pair + _1, rows, units] = cn
            hch[p, rows, units] = hn
        swap(_1 - j, _0).start()
        swap(_1 - j, _1).start()

    def up_product(k, at):
        prea[pl.ds(at, PAIRS)] = (mm(hbuf[k], wup[...]) + gate_row(bias_ref, _1)).reshape(PAIRS, 8, wide)

    def again(make, k, fresh):
        @pl.when(fresh)
        def _():
            make(k - _1).wait_send()
        make(k).start()

    def low_copy(i):
        return lambda k: low_send(k, i)

    def up_copy(p):
        return lambda k: up_send(k, p)

    low_turns = ((_1,), (_2,), ('up', _1), ('up', _2), ('up', 3), (3,), (4,), (5, 6))

    def turn(k, e):
        q = k - _1

        @pl.when((x == _0) & (q >= _0))
        def _():
            if low_turns[e][_0] == 'up':
                up_copy(low_turns[e][_1])(q).start()
            else:
                for i in low_turns[e]:
                    again(low_copy(i), q, q >= _1)

        if e < 7:
            @pl.when((x == _1) & (q >= _0))
            def _():
                again(lambda kk: top_send(kk, e), q, q >= _1)

    def act_out(k):
        rows = pl.ds(k * PAIRS, PAIRS)
        return local(actv.at[rows], act_hbm.at[rows], osem.at[_0])

    def slot_body(s, _):
        k = s - x
        live = (k >= _0) & (k < nch)
        final = (x == _0) & (s == nch)
        upper = (x == _1) & live

        @pl.when(upper)
        def _():
            hrecv(k, c).wait_recv()

        @pl.when(upper | final)
        def _():
            q = x * k + (_1 - x) * (nch - _1)
            hrecv(q, _1 - c).wait_recv()

            @pl.when(final)
            def _():
                for i in (_1, _2):
                    again(low_copy(i), nch - _1, True)
                for p in range(PAIRS):
                    up_send(nch - _2, p).wait_send()
            up_product(q, x * k * PAIRS + (_1 - x) * npair)

            @pl.when(final)
            def _():
                for p in range(PAIRS):
                    up_send(nch - _1, p).start()
                for i in range(3, 7):
                    again(low_copy(i), nch - _1, True)

        @pl.when(live)
        def _():
            @pl.when(x == _0)
            def _():
                pre_load(k).wait()

            up_send(k, _0).wait_recv()
            step(k, _0, _0, lambda: turn(k, _0))

            @pl.when((x == _0) & (k >= _1))
            def _():
                hrecv(k - _1, _1 - c).wait_recv()

                @pl.when(k >= _2)
                def _():
                    for p in range(PAIRS):
                        up_send(k - _2, p).wait_send()
                up_product(k - _1, npair)
                up_send(k - _1, _0).start()

            step(k, _0, _1, lambda: turn(k, _1))

            def pair_body(p, _):
                def turn_of(j):
                    for pp in range(_1, PAIRS):
                        @pl.when(p == pp)
                        def _():
                            turn(k, _2 * pp + j)

                up_send(k, p).wait_recv()
                step(k, p, _0, lambda: turn_of(_0))
                step(k, p, _1, lambda: turn_of(_1))
                return _0

            lax.fori_loop(_1, PAIRS, pair_body, _0)
            act_out(k).start()

            @pl.when(x == _0)
            def _():
                block = hch[...].reshape(ROWS, half).astype(BF16)
                histv[k] = block
                hbuf[k, :, own_cols] = block

                again(low_copy(_0), k, k >= _1)

            @pl.when(x == _1)
            def _():
                block = hch[...].reshape(ROWS, half).astype(BF16)
                histv[k, :, _0:hl] = block[:, hl:half]
                histv[k, :, hl:half] = block[:, _0:hl]

                own_top(k).start()
        return _0

    lax.fori_loop(_0, nch + _1, slot_body, _0)
    local(cellv, cell_hbm, osem.at[_2]).start()
    swap(_0, _0).wait()
    swap(_0, _1).wait()
    last_ref[...] = histv[nch - _1]
    for s in BOTH:
        fin_ref[s, _0] = hch[PAIRS - _1, 4:8, part(s, hl)]
        fin_ref[s, _1] = cst[:, part(s, hl)]

    sent = pl.ds(_0, (nch - _1) * ROWS)

    @pl.when(x == _0)
    def _():
        for i in range(7):
            low_send(nch - _1, i).wait_send()
        for p in range(PAIRS):
            up_send(nch - _1, p).wait_send()
        whole = town_hbm.at[sent, :]
        local(whole, whole, csem.at[_1]).wait()

    @pl.when(x == _1)
    def _():
        for i in range(7):
            top_send(nch - _2, i).wait_send()
        local(pre_hbm, pre_hbm, fsem.at[_0]).wait()
        part = town_hbm.at[sent, pl.ds(_0, half)]
        local(part, part, csem.at[_1]).wait()
        mine = town_hbm.at[:, pl.ds(_0, half)]
        local(mine, mine, osem.at[3]).wait()

    def low_out(k):
        return local(hbuf.at[k], lown_hbm.at[aligned(k, ROWS), :], osem.at[_1])

    def low_start(k, _):
        low_out(k).start()
        return _0

    lax.fori_loop(_0, nch, low_start, _0)
    local(loth_hbm, loth_hbm, csem.at[_0]).wait()
    far = toth_hbm.at[sent, :]
    local(far, far, csem.at[_2]).wait()
    x_send().wait()
    local(lown_hbm, lown_hbm, osem.at[_1]).wait()
    local(cellv, cell_hbm, osem.at[_2]).wait()
    local(actv, act_hbm, osem.at[_0]).wait()


def bwd_kernel(wta_hbm, wtb_hbm, wupt_hbm, act_hbm, cell_hbm, gy_hbm, last_ref, fin_ref,
               dg_hbm, tlo_hbm, tlf_hbm, bias_ref, hfin_ref, cfin_ref,
               wt, wupt, actv, cellv, dout, gyv, dgv, dgr, dgch, dgs, dct, bacc, own, snd, rcv, pin, pout, bsnd, brcv, finr,
               lsem, asem, osem, xs, xr, gs, grs, ps, prs, csem, bsem, tsem):
    y, m, x, c = place()
    beside, across, skew = flips(m)
    nch = dgv.shape[_0]
    half = dct.shape[_1]
    hl = half // _2
    wide = 4 * hl
    hp = PAIRS // _2
    hr = ROWS // _2

    first_loads = [local(cell_hbm, cellv, lsem.at[12])]
    loads = []
    for pos, shard in enumerate((beside, skew, m, across)):
        for row, src in enumerate((wta_hbm, wtb_hbm)):
            loads.append(local(src.at[:, aligned(shard, hl)], wt.at[pl.ds(row * wide, wide), pl.ds(pos * hl, hl)],
                               lsem.at[len(loads)]))
    up_loads = [local(wupt_hbm.at[:, aligned(shard, hl)], wupt.at[:, pl.ds(pos * hl, hl)], lsem.at[8 + pos])
                for pos, shard in enumerate((_1 - c, 3 - c, c, _2 + c))]

    def act_in(k):
        rows = pl.ds(k * PAIRS, PAIRS)
        return local(act_hbm.at[rows], actv.at[rows], asem.at[k])

    @pl.when(x == _1)
    def _():
        local(gy_hbm, gyv, lsem.at[13]).start()
    for cp in first_loads:
        cp.start()
    act_in(nch - _1).start()
    for cp in loads + up_loads:
        cp.start()

    def start_act(i, _):
        act_in(nch - _2 - i).start()
        return _0

    lax.fori_loop(_0, nch - _1, start_act, _0)
    entry_barrier(y, m)

    own_cols = pl.ds(pl.multiple_of(c * half, half), half)

    def last_sends():
        return [remote(last_ref, (tlo_hbm if i < 3 else tlf_hbm).at[:, own_cols], tsem.at[i],
                       tsem.at[9] if i < 3 else tsem.at[10], dev(oy, om))
                for i, (oy, om) in enumerate(everyone(y, m))]

    def last_keep():
        return local(last_ref, tlo_hbm.at[:, own_cols], tsem.at[11])

    def fin_send():
        return remote(fin_ref.at[_1], finr, tsem.at[7], tsem.at[8], dev(y, across))

    @pl.when(x == _1)
    def _():
        for cp in last_sends():
            cp.start()
        last_keep().start()
    fin_send().start()

    def swap(slot):
        return remote(snd.at[slot], rcv.at[slot], xs.at[slot], xr.at[slot], dev(y, beside))

    part_a = pl.ds(_0, wide)
    part_b = pl.ds(wide, wide)

    def half_rows(k, h):
        return pl.ds(pl.multiple_of(k * ROWS, ROWS) + h * hr, hr)

    def up_grads(k, h):
        rows = pl.ds(h * hr, hr)
        return remote(dgv.at[k, rows, part_b], dgr.at[k, rows], gs.at[_0, h], grs.at[k, h], dev(y, across))

    def near(k, h, top):
        if top:
            return up_grads(k, h)
        return remote(dgv.at[k, pl.ds(h * hr, hr), part_b], dg_hbm.at[_0, _0, half_rows(k, h), :],
                      gs.at[_0, h], csem.at[_2], dev(y, across))

    def wider(k, h, top):
        rows = pl.ds(h * hr, hr)
        layer = _1 if top else _0
        dst = dg_hbm.at[layer, _1, half_rows(k, h), :]
        return (remote(dgv.at[k, rows, part_a], dst, gs.at[_1, h], csem.at[_0], dev(_1 - y, m)),
                remote(dgv.at[k, rows, part_b], dst, gs.at[_2, h], csem.at[_1], dev(_1 - y, across)))

    def keep(k, h, top):
        return local(dgv.at[k, pl.ds(h * hr, hr), part_a], dg_hbm.at[_1 if top else _0, _0, half_rows(k, h), :], osem.at[_0])

    def keep_up(k):
        return local(dgr.at[k], dg_hbm.at[_1, _0, aligned(k, ROWS), :], osem.at[_1])

    def psend(k, pos, piece, dest, src):
        rows = pl.ds(piece * hp, hp)
        return remote(pout.at[pos, rows], pin.at[src, k, rows], ps.at[pos, piece], prs.at[src, k, piece], dev(y, dest))

    def up_sends(k, pos):
        return [psend(k, pos, piece, skew if pos == _0 else across, c) for piece in (_1, _0)]

    def side_sends(k):
        return [psend(k, _0, piece, beside, _2) for piece in (_1, _0)]

    dct[...] = jnp.zeros(dct.shape, F32)
    bacc[...] = jnp.zeros(bacc.shape, F32)

    @pl.when(x == _1)
    def _():
        local(gy_hbm, gyv, lsem.at[13]).wait()
        for s in BOTH:
            dout[:, :, part(s, hl)] = gyv[s].astype(F32).reshape(nch * PAIRS, 8, hl)

    @pl.when(x == _0)
    def _():
        for cp in up_loads:
            cp.wait()
    for cp in first_loads:
        cp.wait()

    def point(k, p, j, inner):
        pair = k * PAIRS + p
        rows = part(j, BATCH)
        for s in BOTH:
            base = s * wide
            units = part(s, hl)
            gi, gf, go, gu = (actv[pair, rows, part(g, hl, base)] for g in GATES)
            tc = jnp.tanh(cellv[pair + _1, rows, units])
            cp = cellv[pair + _1, _0:4, units] if j else cellv[pair, 4:8, units]
            dh = dout[pair, rows, units]
            if inner:
                dh = dh + own[:, units] + rcv[j, :, units]
            dc = dct[:, units] + dh * go * (1.0 - tc * tc)
            dct[:, units] = dc * gf
            grads = (dc * gu * gi * (1.0 - gi), dc * cp * gf * (1.0 - gf),
                     dh * tc * go * (1.0 - go), dc * gi * (1.0 - gu * gu))
            for g, val in enumerate(grads):
                cols = part(g, hl, base)
                dgs[:, cols] = val.astype(BF16)
                dgch[p, rows, cols] = val

    def step(k, p, j, after):
        dgl = dgs[...]
        snd[j] = mm(dgl, wt[:, _0:half])
        swap(j).start()
        own[...] = mm(dgl, wt[:, half:])
        swap(j).wait()
        after()
        point(k, p, j, True)

    def again(make, k):
        @pl.when(k < nch - _1)
        def _():
            make(k + _1).wait_send()
        make(k).start()

    def near_copy(h, top):
        return lambda k: near(k, h, top)

    def wide_copy(h, top, i):
        return lambda k: wider(k, h, top)[i]

    def turn(k, e):
        late = k < nch - _1

        if e < 3:
            @pl.when((x == _0) & late)
            def _():
                again((near_copy(_0, False), wide_copy(_0, False, _0), wide_copy(_0, False, _1))[e], k + _1)
        if e in (4, 5, 6):
            @pl.when(x == _0)
            def _():
                again((near_copy(_1, False), wide_copy(_1, False, _0), wide_copy(_1, False, _1))[e - 4], k)
        if e < _2:
            @pl.when((x == _1) & late)
            def _():
                up_sends(k + _1, e)[_1].start()
        if e in (_2, 3):
            @pl.when((x == _1) & late)
            def _():
                again(wide_copy(_0, True, e - _2), k + _1)
        if e in (5, 6):
            @pl.when(x == _1)
            def _():
                again(wide_copy(_1, True, e - 5), k)

    def emit(k, h):
        dgv[k, part(h, hr), :] = dgch[part(h, hp)].reshape(hr, _2 * wide).astype(BF16)
        total = dgch[h * hp]
        for p in range(h * hp + _1, (h + _1) * hp):
            total = total + dgch[p]
        bacc[...] += total

        @pl.when(x == _0)
        def _():
            keep(k, h, False).start()

        @pl.when(x == _1)
        def _():
            again(near_copy(h, True), k)
            keep(k, h, True).start()

    def take(k, piece):
        for src in (_0, _1, _2):
            psend(k, _0, piece, beside, src).wait_recv()
        rows = pl.ds(piece * hp, hp)
        dout[pl.ds(k * PAIRS + piece * hp, hp)] = pout[_1, rows] + pin[_0, k, rows] + pin[_1, k, rows] + pin[_2, k, rows]

    def slot_body(s, _):
        k = nch - _1 - s + (_1 - x)
        live = (k >= _0) & (k < nch)
        first = live & (k == nch - _1)

        @pl.when((x == _0) & live)
        def _():
            @pl.when(k < nch - _1)
            def _():
                for cp in side_sends(k + _1):
                    cp.wait_send()
            up_grads(k, _1).wait_recv()
            up_grads(k, _0).wait_recv()
            keep_up(k).start()
            block = dgr[k]
            pout[_0] = mm(block, wupt[:, _0:half]).reshape(PAIRS, 8, half)
            for cp in side_sends(k):
                cp.start()
            pout[_1] = mm(block, wupt[:, half:]).reshape(PAIRS, 8, half)
            take(k, _1)

        @pl.when(live)
        def _():
            act_in(k).wait()

            @pl.when(first)
            def _():
                point(k, PAIRS - _1, _1, False)
                for cp in loads:
                    cp.wait()

                @pl.when(x == _1)
                def _():
                    for cp in up_loads:
                        cp.wait()

            @pl.when(k < nch - _1)
            def _():
                step(k, PAIRS - _1, _1, lambda: turn(k, _0))
            step(k, PAIRS - _1, _0, lambda: turn(k, _1))

            def pair_body(i, _):
                p = PAIRS - _2 - i

                @pl.when((x == _0) & (p == hp - _1))
                def _():
                    take(k, _0)

                def turn_of(j):
                    for pp in range(PAIRS - _1):
                        @pl.when(p == pp)
                        def _():
                            turn(k, _2 * (PAIRS - _1 - pp) + _1 - j)

                step(k, p, _1, lambda: turn_of(_1))
                step(k, p, _0, lambda: turn_of(_0))

                @pl.when(p == hp)
                def _():
                    emit(k, _1)
                return _0

            lax.fori_loop(_0, PAIRS - _1, pair_body, _0)
            emit(k, _0)

        @pl.when((x == _1) & live)
        def _():
            @pl.when(k < nch - _1)
            def _():
                for pos in BOTH:
                    for cp in up_sends(k + _1, pos):
                        cp.wait_send()
            block = dgv[k, :, _0:wide]
            for pos in BOTH:
                pout[pos] = mm(block, wupt[:, part(pos, half)]).reshape(PAIRS, 8, half)
                up_sends(k, pos)[_0].start()
        return _0

    lax.fori_loop(_0, nch + _1, slot_body, _0)

    @pl.when(x == _0)
    def _():
        again(near_copy(_0, False), _0)
        for i in BOTH:
            again(wide_copy(_0, False, i), _0)

    @pl.when(x == _1)
    def _():
        for pos in BOTH:
            up_sends(_0, pos)[_1].start()
        for i in BOTH:
            again(wide_copy(_0, True, i), _0)

    bsnd[_0] = bacc[:, _0:wide]
    bsnd[_1] = bacc[:, wide:]
    shares = (remote(bsnd.at[_0], brcv.at[_0], bsem.at[_0], bsem.at[3], dev(_1 - y, m)),
              remote(bsnd.at[_1], brcv.at[_1], bsem.at[_1], bsem.at[4], dev(y, across)),
              remote(bsnd.at[_1], brcv.at[_2], bsem.at[_2], bsem.at[5], dev(_1 - y, across)))
    for cp in shares:
        cp.start()

    fin_send().wait()
    for ref, i in ((hfin_ref, _0), (cfin_ref, _1)):
        ref[_0] = jnp.where(x == _0, fin_ref[_0, i], finr[i])
        ref[_1] = jnp.where(x == _0, finr[i], fin_ref[_0, i])

    quarter = dg_hbm.at[_0, _0]

    @pl.when(x == _0)
    def _():
        for cp in side_sends(_0):
            cp.wait_send()
        for h in BOTH:
            near(_0, h, False).wait_send()
            for cp in wider(_0, h, False):
                cp.wait_send()
        local(quarter, quarter, osem.at[_1]).wait()
        local(tlo_hbm, tlo_hbm, tsem.at[9]).wait()

    @pl.when(x == _1)
    def _():
        for pos in BOTH:
            for cp in up_sends(_0, pos):
                cp.wait_send()
        for h in BOTH:
            near(_0, h, True).wait_send()
            for cp in wider(_0, h, True):
                cp.wait_send()
        local(quarter, quarter, csem.at[_2]).wait()
        for cp in last_sends():
            cp.wait_send()
        local(last_ref, last_ref, tsem.at[9]).wait()
        last_keep().wait()

    local(tlf_hbm, tlf_hbm, tsem.at[10]).wait()
    local(quarter, quarter, csem.at[_0]).wait()
    local(quarter, quarter, csem.at[_1]).wait()
    local(quarter, quarter, osem.at[_0]).wait()
    for cp in shares:
        cp.wait()
    same = jnp.sum(bsnd[_0] + brcv[_0], axis=_0, keepdims=True)
    cross = jnp.sum(brcv[_1] + brcv[_2], axis=_0, keepdims=True)
    low = jnp.where(x == _0, same, cross)
    top = jnp.where(x == _0, cross, same)
    for g in GATES:
        bias_ref[_0, g:g + _1, :] = low[:, part(g, hl)]
        bias_ref[_1, g:g + _1, :] = top[:, part(g, hl)]


def grad_kernel(xo_hbm, xf_hbm, lo_hbm, lf_hbm, to_hbm, tf_hbm, tlo_hbm, tlf_hbm, init_ref, dg_hbm,
                dwin_hbm, dwup_hbm, dwrec_hbm, y_ref,
                lhs, grads, htop, shf, yf, lhst0, lhst1, pieces0, pieces1, lsem, osem):
    hidden = htop.shape[_1]
    srows = lo_hbm.shape[_0]
    lhst = (lhst0, lhst1)
    pieces = (pieces0, pieces1)
    kb = lhst0.shape[_0]
    hl = hidden // 4
    nblk = hidden // kb
    per = hl // LANES
    nq = hl // kb
    m = lax.axis_index('model')
    x = m // _2
    c = m % _2
    lo = pl.ds(_0, srows)
    hi = pl.ds(srows, srows)
    body_rows = pl.ds(_0, srows - ROWS)
    srcs = ((xo_hbm, lhs.at[_0, lo, :]), (xf_hbm, lhs.at[_0, hi, :]), (dg_hbm.at[_0, _0], grads.at[_0, lo, :]), (dg_hbm.at[_0, _1], grads.at[_0, hi, :]),
            (lo_hbm, lhs.at[_1, lo, :]), (lf_hbm, lhs.at[_1, hi, :]), (dg_hbm.at[_1, _0], grads.at[_1, lo, :]), (dg_hbm.at[_1, _1], grads.at[_1, hi, :]),
            (to_hbm.at[body_rows, :], htop.at[body_rows, :]),
            (tf_hbm.at[body_rows, :], htop.at[pl.ds(srows, srows - ROWS), :]),
            (tlo_hbm, htop.at[pl.ds(srows - ROWS, ROWS), :]), (tlf_hbm, htop.at[pl.ds(_2 * srows - ROWS, ROWS), :]))
    loads = [local(a, b, lsem.at[i]) for i, (a, b) in enumerate(srcs)]
    for cp in loads:
        cp.start()

    def core_row(i):
        q = i // nq
        return ((q % _2) * _2 + q // _2) * nq + i % nq

    def out_start(slot, n):
        ph = n // nblk
        i = lax.rem(n, nblk)

        def put(dst, off):
            for j in range(4 * per):
                local(pieces[slot].at[j], dst.at[aligned(off, kb), j, :], osem.at[slot]).start()

        @pl.when(ph == _0)
        def _():
            put(dwin_hbm, i)

        @pl.when(ph == _1)
        def _():
            put(dwup_hbm, core_row(i))

        @pl.when(ph >= _2)
        def _():
            put(dwrec_hbm, (ph - _2) * nblk + core_row(i))

    def out_wait(slot):
        local(pieces[slot], pieces[slot], osem.at[slot]).wait()

    def shift(src, dst, layer, i):
        cols = aligned(i, kb)
        for part in BOTH:
            base = part * srows
            shf[base + 4:base + srows, :] = src[pl.ds(base, srows), cols].astype(F32)[:srows - 4]
            shf[base:base + 4, :] = init_ref[layer, part, :, cols].astype(F32)
        dst[:, cols] = shf[...].astype(BF16)

    def prepare(slot, n):
        lhst[slot][...] = lhs[n // nblk, :, aligned(lax.rem(n, nblk), kb)].T

    total = 4 * nblk
    for cp in loads[_0:4]:
        cp.wait()
    prepare(_0, _0)

    def body(it, _):
        @pl.when(it == nblk // _2 - _1)
        def _():
            for cp in loads[4:]:
                cp.wait()

        @pl.when((it >= nblk // _2) & (it < nblk))
        def _():
            for e in BOTH:
                i = _2 * it + e - nblk
                shift(lhs.at[_1], lhs.at[_2], _0, i)
                shift(htop, lhs.at[3], _1, i)

        for e in BOTH:
            n = _2 * it + e

            @pl.when(n >= _2)
            def _():
                out_wait(e)
            res = mm(lhst[e][...], grads[lax.rem(n // nblk, _2)])
            for g in GATES:
                for ct in range(per):
                    col = g * hl + ct * LANES
                    pieces[e][ct * 4 + g] = res[:, col:col + LANES]
            prepare(_1 - e, jnp.minimum(n + _1, total - _1))
            out_start(e, n)
        return _0

    lax.fori_loop(_0, total // _2, body, _0)
    for t in range(per):
        yf[t] = htop[_0:srows, pl.ds(pl.multiple_of(c * _2 * hl + x * hl + t * LANES, LANES), LANES)].astype(F32)
        for b in range(BATCH):
            y_ref[b, :, part(t, LANES)] = yf[t, pl.ds(b, srows // BATCH, stride=BATCH), :].astype(BF16)
    for slot in BOTH:
        out_wait(slot)


def any_spec():
    return pl.BlockSpec(memory_space=pl.ANY)


def vmem_spec():
    return pl.BlockSpec(memory_space=pltpu.VMEM)


def sds(shape, dtype):
    return jax.ShapeDtypeStruct(shape, dtype)


DMA = pltpu.SemaphoreType.DMA


def comm_params(i):
    return pltpu.CompilerParams(collective_id=i, has_side_effects=True, vmem_limit_bytes=VMEM_LIMIT)


def run_prep(wrec, wup, win, x, gy, hc, bias):
    batch, seq, width = x.shape
    hl = gy.shape[_2]
    wide = 4 * hl
    hidden = 4 * hl
    rows = batch * seq
    raw = win.shape[_0]
    per = hl // LANES
    span = KB * 4 * per
    square = sds((hidden, wide), BF16)
    vm = pltpu.VMEM
    return pl.pallas_call(
        prep_kernel,
        name='lstm_prepare',
        out_shape=(square,) * 6 + (sds((rows // 8, 8, wide), F32), sds((rows, width), BF16), sds((_2, rows, hl), BF16),
                                   sds((_2, 4, hl), F32), sds((_2, _2, 4, hidden), BF16)),
        in_specs=[any_spec()] * 5 + [vmem_spec()] * _2,
        out_specs=(any_spec(),) * 9 + (vmem_spec(),) * _2,
        scratch_shapes=[
            vm((raw, LANES), BF16), vm((raw, LANES), BF16), vm((raw, LANES), BF16), vm((raw, LANES), BF16),
            vm((_2, span, LANES), F32), vm((6, KB, wide), BF16), vm((6, wide, KB), BF16), vm((width, wide), BF16),
            vm(x.shape, BF16), vm((4, rows, LANES), F32), vm((rows, width), BF16), vm((rows // 8, 8, wide), F32),
            vm(gy.shape, BF16), vm((rows, hl), BF16), vm((_2, 4, hl), BF16),
            vm((_2, _2, 4, hidden), BF16), vm((_2, 4, hl), F32),
            DMA((5,)), DMA((3,)), DMA((6, _2)), DMA((NX,)), DMA((NX,)), DMA((NX,)), DMA((NX,)), DMA((8,)), DMA((8,)), DMA((_2,)),
        ],
        compiler_params=comm_params(_0),
    )(wrec, wup, win, x, gy, hc, bias)


def run_fwd(wa, wb, wup, pre, xt, hc, hcb, bias):
    hidden, wide = wa.shape
    hl = wide // 4
    half = _2 * hl
    npair = pre.shape[_0]
    nch = npair // PAIRS
    rows = npair * 8
    hist = sds((rows, hidden), BF16)
    vm = pltpu.VMEM
    return pl.pallas_call(
        fwd_kernel,
        name='lstm_forward',
        out_shape=(sds((npair, 8, _2 * wide), F32), sds((npair + _1, 8, half), F32), hist, hist, hist, hist,
                   sds(xt.shape, BF16), sds((ROWS, half), BF16), sds((_2, _2, 4, hl), F32)),
        in_specs=[any_spec()] * 5 + [vmem_spec()] * 3,
        out_specs=(any_spec(),) * 7 + (vmem_spec(),) * _2,
        scratch_shapes=[
            vm((hidden, _2 * wide), BF16), vm((hidden, wide), BF16),
            vm((npair + PAIRS, 8, wide), F32), vm((npair, 8, wide), F32),
            vm((npair, 8, _2 * wide), F32), vm((npair + _1, 8, half), F32),
            vm((nch, ROWS, half), BF16), vm((nch, ROWS, hidden), BF16),
            vm((PAIRS, 8, half), F32), vm((4, half), F32),
            vm((_2, _2, 4, hl), BF16), vm((_2, _2, 4, hl), BF16),
            DMA((12,)), DMA((nch,)), DMA((4,)), DMA((_2, _2)), DMA((_2, _2)), DMA((7,)), DMA((nch, _2)),
            DMA((PAIRS,)), DMA((npair,)), DMA((3,)), DMA((3,)),
        ],
        compiler_params=comm_params(_1),
    )(wa, wb, wup, pre, xt, hc, hcb, bias)


def run_bwd(wta, wtb, wupt, act, cell, gy, last, fin):
    wide, hidden = wta.shape
    hl = wide // 4
    half = _2 * hl
    npair = act.shape[_0]
    nch = npair // PAIRS
    rows = npair * 8
    vm = pltpu.VMEM
    state = sds((_2, 4, hl), F32)
    return pl.pallas_call(
        bwd_kernel,
        name='lstm_backward',
        out_shape=(sds((_2, _2, rows, wide), BF16), sds((ROWS, hidden), BF16), sds((ROWS, hidden), BF16), state, state, state),
        in_specs=[any_spec()] * 6 + [vmem_spec()] * _2,
        out_specs=(any_spec(),) * 3 + (vmem_spec(),) * 3,
        scratch_shapes=[
            vm((_2 * wide, hidden), BF16), vm((wide, hidden), BF16),
            vm((npair, 8, _2 * wide), F32), vm((npair + _1, 8, half), F32),
            vm((npair, 8, half), F32), vm((_2, rows, hl), BF16),
            vm((nch, ROWS, _2 * wide), BF16), vm((nch, ROWS, wide), BF16),
            vm((PAIRS, 8, _2 * wide), F32), vm((4, _2 * wide), BF16),
            vm((4, half), F32), vm((8, _2 * wide), F32),
            vm((4, half), F32), vm((_2, 4, half), F32), vm((_2, 4, half), F32),
            vm((3, nch, PAIRS, 8, half), F32), vm((_2, PAIRS, 8, half), F32),
            vm((_2, 8, wide), F32), vm((3, 8, wide), F32), vm((_2, 4, hl), F32),
            DMA((14,)), DMA((nch,)), DMA((_2,)), DMA((_2,)), DMA((_2,)), DMA((3, _2)), DMA((nch, _2)), DMA((_2, _2)), DMA((3, nch, _2)),
            DMA((3,)), DMA((6,)), DMA((12,)),
        ],
        compiler_params=comm_params(_2),
    )(wta, wtb, wupt, act, cell, gy, last, fin)


def run_grads(xo, xf, lo, lf, to, tf, tlo, tlf, init, dg):
    srows, hidden = lo.shape
    rows = _2 * srows
    wide = dg.shape[3]
    tile = (wide // LANES, LANES)
    hl = wide // 4
    kb = 512
    vm = pltpu.VMEM
    return pl.pallas_call(
        grad_kernel,
        name='weight_grads',
        out_shape=(sds((hidden,) + tile, F32), sds((hidden,) + tile, F32), sds((_2 * hidden,) + tile, F32),
                   sds((BATCH, srows // BATCH, hl), BF16)),
        in_specs=[any_spec()] * 8 + [vmem_spec(), any_spec()],
        out_specs=(any_spec(),) * 3 + (vmem_spec(),),
        scratch_shapes=[vm((4, rows, hidden), BF16), vm((_2, rows, wide), BF16), vm((rows, hidden), BF16),
                        vm((rows, kb), F32), vm((hl // LANES, srows, LANES), F32), vm((kb, rows), BF16), vm((kb, rows), BF16),
                        vm((wide // LANES, kb, LANES), F32), vm((wide // LANES, kb, LANES), F32), DMA((12,)), DMA((_2,))],
        compiler_params=pltpu.CompilerParams(vmem_limit_bytes=VMEM_LIMIT),
    )(xo, xf, lo, lf, to, tf, tlo, tlf, init, dg)


def to_raw(w):
    hl = w.shape[-_1]
    w = w.reshape(-_1, 4, hl // LANES, LANES)
    return jnp.swapaxes(w, _1, _2).reshape(-_1, LANES)


def from_raw(v, lead, hl):
    v = v.reshape(-_1, hl // LANES, 4, LANES)
    return jnp.swapaxes(v, _1, _2).reshape(lead + (-_1, 4, hl))


def solution(mesh):
    batch_axes = ('part', 'data')
    seq_spec = P(batch_axes, None, 'model')
    state_spec = P(None, batch_axes, 'model')
    weight_spec = P(None, None, None, 'model')
    in_specs = (P(batch_axes, None, None), seq_spec, state_spec, state_spec,
                P(None, None, 'model'), weight_spec, weight_spec, P(None, None, 'model'))
    out_specs = (seq_spec, state_spec, state_spec, P('part', None, 'model'),
                 P(None, 'part', None, 'model'), P(None, 'part', None, 'model'), P(None, 'part', 'model'))

    def local_program(x_seq, gy_seq, h_init, c_init, w_in, w_up, w_rec, gate_bias):
        hl = w_in.shape[_2]
        hc = jnp.stack([h_init, c_init], axis=_1)
        wa, wb, wat, wbt, wup, wupt, pre, xt, gyt, hcb, init = run_prep(
            to_raw(w_rec), to_raw(w_up), to_raw(w_in), x_seq, gy_seq, hc, gate_bias)
        act, cell, low_own, low_far, top_own, top_far, x_far, last, fin = run_fwd(
            wa, wb, wup, pre, xt, hc, hcb, gate_bias)
        dg, last_own, last_far, bias, h_last, c_last = run_bwd(wat, wbt, wupt, act, cell, gyt, last, fin)
        dw_in, dw_up, dw_rec, y_out = run_grads(
            xt, x_far, low_own, low_far, top_own, top_far, last_own, last_far, init, dg)
        return (y_out, h_last, c_last, from_raw(dw_in, (), hl), from_raw(dw_up, (_1,), hl),
                from_raw(dw_rec, (_2,), hl), bias)

    return jax.shard_map(local_program, mesh=mesh, in_specs=in_specs, out_specs=out_specs, check_vma=False)
```

```python
import jax
import jax.numpy as jnp
from jax import lax
from jax.experimental import pallas as pl
from jax.experimental.pallas import tpu as pltpu
from jax.sharding import PartitionSpec as P

MESH = pl.DeviceIdType.MESH
F32 = jnp.float32
BF16 = jnp.bfloat16
LANES = 128
BATCH = 4
CHUNK = 8
_0, _1, _2 = range(3)
BOTH = (_0, _1)
GATES = range(4)
PAIRS = CHUNK // _2
ROWS = BATCH * CHUNK
KB = 128
NX = 8
AHEAD = 4
VMEM_LIMIT = 63 * 1024 * 1024
STEP_LIMIT = 37 * 1024 * 1024


def sigm(v):
    return 0.5 * jnp.tanh(0.5 * v) + 0.5


def mm(a, b):
    return jnp.dot(a, b, preferred_element_type=F32)


def place():
    y = lax.axis_index('data')
    m = lax.axis_index('model')
    return y, m, m // _2, m % _2


def dev(y, m):
    return (lax.axis_index('part'), y, m)


def flips(m):
    x = m // _2
    c = m % _2
    return _2 * x + (_1 - c), _2 * (_1 - x) + c, _2 * (_1 - x) + (_1 - c)


def everyone(y, m):
    beside, across, skew = flips(m)
    return ((y, beside), (y, across), (y, skew), (_1 - y, m), (_1 - y, beside), (_1 - y, across), (_1 - y, skew))


def remote(src, dst, ssem, rsem, device):
    return pltpu.make_async_remote_copy(src, dst, ssem, rsem, device_id=device, device_id_type=MESH)


def local(src, dst, sem):
    return pltpu.make_async_copy(src, dst, sem)


def entry_barrier(y, m):
    barrier = pltpu.get_barrier_semaphore()
    for oy, om in everyone(y, m):
        pl.semaphore_signal(barrier, inc=_1, device_id=dev(oy, om), device_id_type=MESH)
    pl.semaphore_wait(barrier, 7)


def part(i, n, base=_0):
    return slice(base + i * n, base + (i + _1) * n)


def aligned(i, n):
    return pl.ds(pl.multiple_of(i * n, n), n)


def gate_row(bias_ref, layer):
    return jnp.concatenate([bias_ref[layer, g:g + _1, :] for g in GATES], axis=_1)


def prep_kernel(wrec_hbm, wup_hbm, win_hbm, x_hbm, gy_hbm, h_ref, c_ref, bias_ref,
                wa_hbm, wb_hbm, wat_hbm, wbt_hbm, wup2_hbm, wupt_hbm, pre_hbm, xt_hbm, gyt_hbm, hcb_ref, init_ref,
                rin, rup, ra, rb, spread, wst, wtst, win, xin, xf, xb, prev, gyin, gyb, ib, initv, hcv,
                lsem, osem, jsem, ssx, rsx, ssy, rsy, sss, rss, gsem):
    y, m, x, c = place()
    beside, across, skew = flips(m)
    hl = h_ref.shape[_2]
    per = hl // LANES
    stride = 4 * per
    span = KB * stride
    seq = xin.shape[_1]
    whole = rb.shape[_0]
    part_rows = whole // _2

    loads = [local(x_hbm, xin, lsem.at[_0]),
             local(win_hbm, rin, lsem.at[_1]),
             local(wrec_hbm.at[aligned(x, whole), :], ra, lsem.at[_2]),
             local(wup_hbm, rup, lsem.at[3]),
             local(gy_hbm, gyin, lsem.at[4])]
    for cp in loads:
        cp.start()
    entry_barrier(y, m)

    def xsend(i):
        off = y * part_rows + i * span
        src = wrec_hbm.at[pl.ds(pl.multiple_of((_1 - x) * whole + off, span), span), :]
        return remote(src, rb.at[pl.ds(pl.multiple_of(off, span), span), :], ssx.at[i], rsx.at[i], dev(y, across))

    def ysend(i):
        rows = pl.ds(pl.multiple_of(y * part_rows + i * span, span), span)
        return remote(rb.at[rows, :], rb.at[rows, :], ssy.at[i], rsy.at[i], dev(_1 - y, m))

    def small(i, dest_y, dest_m):
        slot = _0 if i < 3 else _1
        dst = initv.at[:, slot, :, pl.ds(pl.multiple_of(c * _2 * hl + x * hl, hl), hl)]
        return remote(ib, dst, sss.at[i], rss.at[i], dev(dest_y, dest_m))

    def state_sends():
        return [remote(ref.at[_1 - x], hcv.at[i], sss.at[7 + i], rss.at[7 + i], dev(y, across))
                for i, ref in enumerate((h_ref, c_ref))]

    ib[...] = h_ref[...].astype(BF16)
    initv[:, _0, :, pl.ds(pl.multiple_of(c * _2 * hl + x * hl, hl), hl)] = ib[...]
    for i, (oy, om) in enumerate(everyone(y, m)):
        small(i, oy, om).start()
    for cp in state_sends():
        cp.start()
    for i in range(NX):
        xsend(i).start()

    loads[_0].wait()
    for t in range(xb.shape[_1] // LANES):
        cols = part(t, LANES)
        for b in range(BATCH):
            xf[t % 4, pl.ds(b, seq, stride=BATCH), :] = xin[b, :, cols].astype(F32)
        xb[:, cols] = xf[t % 4].astype(BF16)
    xout = local(xb, xt_hbm, osem.at[_0])
    xout.start()
    loads[4].wait()
    for t in range(per):
        cols = part(t, LANES)
        for b in range(BATCH):
            xf[t % 4, pl.ds(b, seq, stride=BATCH), :] = gyin[b, :, cols].astype(F32)
        gyb[:, cols] = xf[t % 4].astype(BF16)
    gout = local(gyb, gyt_hbm.at[_0], osem.at[_1])
    gout.start()

    def gy_send():
        return remote(gyb, gyt_hbm.at[_1], gsem.at[_0], gsem.at[_1], dev(y, across))

    @pl.when(x == _0)
    def _():
        gy_send().start()

    for cp in loads[_1:4]:
        cp.wait()

    def tiles(buf, raw, blk):
        spread[buf] = raw[aligned(blk, span), :].astype(F32)
        for g in GATES:
            for ct in range(per):
                yield g * hl + ct * LANES, spread[buf, pl.ds(ct * 4 + g, KB, stride=stride), :]

    def job_out(pos, blk, wo, wto):
        return (local(wst.at[pos], wo.at[aligned(blk, KB), :], jsem.at[pos, _0]),
                local(wtst.at[pos], wto.at[:, aligned(blk, KB)], jsem.at[pos, _1]))

    def job(pos, raw, blk, wo, wto):
        for off, tile in tiles(pos % _2, raw, blk):
            wst[pos, :, off:off + LANES] = tile.astype(BF16)
            wtst[pos, off:off + LANES, :] = tile.T.astype(BF16)
        for cp in job_out(pos, blk, wo, wto):
            cp.start()

    def job_wait(pos, wo, wto):
        for cp in job_out(pos, _0, wo, wto):
            cp.wait()

    early = NX // _2

    def body(i, _):
        @pl.when(i < early)
        def _():
            for q in range(4):
                blk = i * 4 + q
                for off, tile in tiles(q % _2, rin, blk):
                    win[aligned(blk, KB), off:off + LANES] = tile.astype(BF16)

        @pl.when(i == early)
        def _():
            row = gate_row(bias_ref, _0)
            nr = KB

            def pre_body(r, _):
                val = mm(xb[aligned(r, nr), :], win[...]) + row
                prev[aligned(r, nr // 8)] = val.reshape(nr // 8, 8, val.shape[_1])
                return _0

            lax.fori_loop(_0, xb.shape[_0] // nr, pre_body, _0)
            local(prev, pre_hbm, osem.at[_2]).start()

        @pl.when(i >= early)
        def _():
            for q in range(4):
                if q < _2:
                    @pl.when(i > early)
                    def _():
                        job_wait(q, wup2_hbm, wupt_hbm)
                else:
                    job_wait(q % _2, wup2_hbm, wupt_hbm)
                job(q % _2, rup, (i - early) * 4 + q, wup2_hbm, wupt_hbm)

        for q in range(_2):
            @pl.when(i > _0)
            def _():
                job_wait(_2 + q, wa_hbm, wat_hbm)
            job(_2 + q, ra, i * _2 + q, wa_hbm, wat_hbm)

        xsend(i).wait_recv()
        ysend(i).start()

        @pl.when(i > _0)
        def _():
            job_wait(4, wb_hbm, wbt_hbm)
        job(4, rb, y * NX + i, wb_hbm, wbt_hbm)

        @pl.when(i > _0)
        def _():
            ysend(i - _1).wait_recv()

            @pl.when(i > _1)
            def _():
                job_wait(5, wb_hbm, wbt_hbm)
            job(5, rb, (_1 - y) * NX + i - _1, wb_hbm, wbt_hbm)
        return _0

    lax.fori_loop(_0, NX, body, _0)
    job_wait(5, wb_hbm, wbt_hbm)
    ysend(NX - _1).wait_recv()
    job(5, rb, (_1 - y) * NX + NX - _1, wb_hbm, wbt_hbm)

    for i, (oy, om) in enumerate(everyone(y, m)):
        small(i, oy, om).wait()
    for cp in state_sends():
        cp.wait()
    hcb_ref[...] = hcv[...]
    init_ref[...] = initv[...]

    @pl.when(x == _0)
    def _():
        gy_send().wait_send()

    @pl.when(x == _1)
    def _():
        gy_send().wait_recv()

    for i in range(NX):
        xsend(i).wait_send()
        ysend(i).wait_send()
    for q in range(_2):
        job_wait(q, wup2_hbm, wupt_hbm)
        job_wait(_2 + q, wa_hbm, wat_hbm)
    job_wait(4, wb_hbm, wbt_hbm)
    job_wait(5, wb_hbm, wbt_hbm)
    xout.wait()
    gout.wait()
    local(prev, pre_hbm, osem.at[_2]).wait()


def fwd_kernel(wa_hbm, wb_hbm, wup_hbm, pre_hbm, xt_hbm, wta_hbm, wtb_hbm, h_ref, c_ref, hcb_ref, bias_ref,
               actv, cellv, wt, lown_hbm, town_hbm, far_hbm, xoth_hbm, last_ref, fin_ref,
               w, wup, prea, preb, histv, hbuf, hch, cst, hs, hr,
               lsem, psem, osem, xs, xr, hss, hrs, ps, prs, csem, fsem):
    y, m, x, c = place()
    beside, across, skew = flips(m)
    nch = hbuf.shape[_0]
    npair = nch * PAIRS
    hl = hs.shape[3]
    half = _2 * hl
    wide = 4 * hl
    own_cols = pl.ds(pl.multiple_of(c * half, half), half)
    others = everyone(y, m)

    loads = []
    for pos, shard in enumerate((m, across, beside, skew)):
        for col, src in enumerate((wa_hbm, wb_hbm)):
            loads.append(local(src.at[aligned(shard, hl), :], w.at[pl.ds(pos * hl, hl), pl.ds(col * wide, wide)],
                               lsem.at[len(loads)]))
    up_loads = [local(wup_hbm.at[pl.ds(shard * hl, hl), :], wup.at[pl.ds(pos * hl, hl), :], lsem.at[8 + pos])
                for pos, shard in enumerate((_0, _2, _1, 3))]
    for cp in loads:
        cp.start()

    def next_loads():
        out = []
        for pos, shard in enumerate((beside, skew, m, across)):
            for row, src in enumerate((wta_hbm, wtb_hbm)):
                out.append(local(src.at[:, aligned(shard, hl)], wt.at[pl.ds(row * wide, wide), pl.ds(pos * hl, hl)],
                                 lsem.at[len(out)]))
        return out

    def pre_load(k):
        rows = pl.ds(k * PAIRS, PAIRS)
        return local(pre_hbm.at[rows], prea.at[rows], psem.at[k])

    @pl.when(x == _0)
    def _():
        def start(k, _):
            pre_load(k).start()
            return _0
        lax.fori_loop(_0, nch, start, _0)

    for cp in up_loads:
        cp.start()

    entry_barrier(y, m)

    def swap(slot, s):
        return remote(hs.at[slot, s], hr.at[slot, s], xs.at[slot, s], xr.at[slot, s], dev(y, beside))

    def pre_send(i):
        return remote(pre_hbm.at[i], preb.at[i], fsem.at[_0], prs.at[i], dev(y, across))

    def up_send(k, p):
        return remote(prea.at[npair + p], preb.at[k * PAIRS + p], ps.at[p], prs.at[k * PAIRS + p], dev(y, across))

    def x_send():
        return remote(xt_hbm, xoth_hbm, fsem.at[_1], fsem.at[_2], dev(_1 - y, m))

    @pl.when(x == _1)
    def _():
        def start(i, _):
            pre_send(i).start()
            return _0
        lax.fori_loop(_0, AHEAD * PAIRS, start, _0)

    x_send().start()

    def low_send(k, i):
        oy, om = others[i]
        return remote(histv.at[k], hbuf.at[k, :, own_cols], hss.at[i], hrs.at[k, c], dev(oy, om))

    def top_send(k, i):
        oy, om = others[i]
        return remote(histv.at[k], town_hbm.at[aligned(k, ROWS), own_cols], hss.at[i], csem.at[_1], dev(oy, om))

    def far_send(k, dx, dc):
        om = _2 * lax.rem(x + dx, _2) + lax.rem(c + dc, _2)
        return remote(histv.at[k], far_hbm.at[x, aligned(k, ROWS), own_cols], hss.at[3 + _2 * dx + dc],
                      csem.at[_2 * x], dev(_1 - y, om))

    def hrecv(k, core):
        cols = pl.ds(pl.multiple_of(core * half, half), half)
        return remote(histv.at[k], hbuf.at[k, :, cols], hss.at[_0], hrs.at[k, core], dev(y, beside))

    def own_top(k):
        return local(histv.at[k], town_hbm.at[aligned(k, ROWS), own_cols], osem.at[3])

    init = [[jnp.where(x == _0, ref[_0], ref[_1]) for ref in (h_ref, c_ref)], hcb_ref]
    for s in BOTH:
        units = part(s, hl)
        hs[_0, s] = init[s][_0].astype(BF16)
        cst[:, units] = init[s][_1]
        cellv[_0, _0:4, units] = init[s][_1]
        cellv[_0, 4:8, units] = init[s][_1]
        swap(_0, s).start()
    for cp in loads:
        cp.wait()
    for cp in up_loads:
        cp.wait()

    def step(k, p, j, between):
        pair = k * PAIRS + p
        rows = part(j, BATCH)
        cols = (slice(_0, wide), slice(wide, _2 * wide))
        acc = [mm(hs[j, _0], w[_0:hl, cols[s]]) + mm(hs[j, _1], w[hl:half, cols[s]]) for s in BOTH]
        swap(j, _0).wait()
        swap(j, _1).wait()
        between()
        got = (hr[j, _0], hr[j, _1])
        acc = [acc[s] + (mm(got[_0], w[half:half + hl, cols[s]]) + mm(got[_1], w[half + hl:, cols[s]])) for s in BOTH]
        for s, pre in ((_0, prea), (_1, preb)):
            base = s * wide
            units = part(s, hl)

            def gate(g):
                return acc[s][:, part(g, hl)] + pre[pair, rows, part(g, hl)]

            gi = sigm(gate(_0))
            gf = sigm(gate(_1))
            go = sigm(gate(_2))
            gu = jnp.tanh(gate(3))
            cn = gf * cst[:, units] + gi * gu
            hn = go * jnp.tanh(cn)
            hs[_1 - j, s] = hn.astype(BF16)
            cst[:, units] = cn
            for g, val in enumerate((gi, gf, go, gu)):
                actv[pair, rows, part(g, hl, base)] = val
            cellv[pair + _1, rows, units] = cn
            hch[p, rows, units] = hn
        swap(_1 - j, _0).start()
        swap(_1 - j, _1).start()

    def again(make, k, fresh):
        @pl.when(fresh)
        def _():
            make(k - _1).wait_send()
        make(k).start()

    def feed(k, p):
        @pl.when((x == _1) & (k + AHEAD < nch))
        def _():
            pre_send((k + AHEAD) * PAIRS + p).start()

    def first_turn(k, j):
        q = k - _1
        if j == _1:
            feed(k, _0)

        if j == _0:
            @pl.when((x == _0) & (q >= _0))
            def _():
                for i in (_1, _2):
                    again(lambda v: low_send(v, i), q, q >= _1)

        @pl.when((x == _1) & (q >= _0))
        def _():
            again(lambda v: top_send(v, j), q, q >= _1)

    def turn(k, p, j):
        q = k - _1
        if j == _1:
            feed(k, p)

        @pl.when((x == _0) & (p == _1) & (q >= _0))
        def _():
            up_send(q, _2 + j).start()

        if j == _0:
            @pl.when((x == _1) & (p == _1) & (q >= _0))
            def _():
                again(lambda v: top_send(v, _2), q, q >= _1)

        @pl.when((p >= _2) & (q >= _0))
        def _():
            again(lambda v: far_send(v, p - _2, j), q, q >= _1)

    def up_product(k, at):
        prea[pl.ds(at, PAIRS)] = (mm(hbuf[k], wup[...]) + gate_row(bias_ref, _1)).reshape(PAIRS, 8, wide)

    def slot_body(s, _):
        k = s - x
        live = (k >= _0) & (k < nch)
        final = (x == _0) & (s == nch)
        upper = (x == _1) & live

        @pl.when(upper)
        def _():
            hrecv(k, c).wait_recv()

        @pl.when(upper | final)
        def _():
            q = x * k + (_1 - x) * (nch - _1)
            hrecv(q, _1 - c).wait_recv()

            @pl.when(final)
            def _():
                for i in (_1, _2):
                    again(lambda v: low_send(v, i), nch - _1, True)
                for p in range(PAIRS):
                    up_send(nch - _2, p).wait_send()
            up_product(q, x * k * PAIRS + (_1 - x) * npair)

            @pl.when(final)
            def _():
                for p in range(PAIRS):
                    up_send(nch - _1, p).start()
                for dx in BOTH:
                    for dc in BOTH:
                        again(lambda v: far_send(v, dx, dc), nch - _1, True)

        @pl.when(live)
        def _():
            @pl.when(x == _0)
            def _():
                pre_load(k).wait()

            @pl.when(k == nch - _1)
            def _():
                for cp in next_loads():
                    cp.start()

            up_send(k, _0).wait_recv()
            step(k, _0, _0, lambda: first_turn(k, _0))

            @pl.when((x == _0) & (k >= _1))
            def _():
                hrecv(k - _1, _1 - c).wait_recv()

                @pl.when(k >= _2)
                def _():
                    for p in range(PAIRS):
                        up_send(k - _2, p).wait_send()
                up_product(k - _1, npair)
                up_send(k - _1, _0).start()
                up_send(k - _1, _1).start()

            step(k, _0, _1, lambda: first_turn(k, _1))

            def pair_body(p, _):
                up_send(k, p).wait_recv()
                step(k, p, _0, lambda: turn(k, p, _0))
                step(k, p, _1, lambda: turn(k, p, _1))
                return _0

            lax.fori_loop(_1, PAIRS, pair_body, _0)
            @pl.when(x == _0)
            def _():
                block = hch[...].reshape(ROWS, half).astype(BF16)
                histv[k] = block
                hbuf[k, :, own_cols] = block

                again(lambda v: low_send(v, _0), k, k >= _1)

            @pl.when(x == _1)
            def _():
                block = hch[...].reshape(ROWS, half).astype(BF16)
                histv[k, :, _0:hl] = block[:, hl:half]
                histv[k, :, hl:half] = block[:, _0:hl]

                own_top(k).start()
        return _0

    lax.fori_loop(_0, nch + _1, slot_body, _0)
    swap(_0, _0).wait()
    swap(_0, _1).wait()
    last_ref[...] = histv[nch - _1]
    for s in BOTH:
        fin_ref[s, _0] = hch[PAIRS - _1, 4:8, part(s, hl)]
        fin_ref[s, _1] = cst[:, part(s, hl)]

    sent = pl.ds(_0, (nch - _1) * ROWS)

    @pl.when(x == _0)
    def _():
        for i in range(3):
            low_send(nch - _1, i).wait_send()
        for dx in BOTH:
            for dc in BOTH:
                far_send(nch - _1, dx, dc).wait_send()
        for p in range(PAIRS):
            up_send(nch - _1, p).wait_send()
        whole = town_hbm.at[sent, :]
        local(whole, whole, csem.at[_1]).wait()

    @pl.when(x == _1)
    def _():
        for i in range(3):
            top_send(nch - _2, i).wait_send()
        for dx in BOTH:
            for dc in BOTH:
                far_send(nch - _2, dx, dc).wait_send()
        local(pre_hbm, pre_hbm, fsem.at[_0]).wait()
        part = town_hbm.at[sent, pl.ds(_0, half)]
        local(part, part, csem.at[_1]).wait()
        mine = town_hbm.at[:, pl.ds(_0, half)]
        local(mine, mine, osem.at[3]).wait()

    def low_out(k):
        return local(hbuf.at[k], lown_hbm.at[aligned(k, ROWS), :], osem.at[_1])

    def low_start(k, _):
        low_out(k).start()
        return _0

    lax.fori_loop(_0, nch, low_start, _0)
    local(far_hbm.at[_0], far_hbm.at[_0], csem.at[_0]).wait()
    far = far_hbm.at[_1, sent, :]
    local(far, far, csem.at[_2]).wait()
    x_send().wait()
    local(lown_hbm, lown_hbm, osem.at[_1]).wait()
    for cp in next_loads():
        cp.wait()


def bwd_kernel(wupt_hbm, gy_hbm, actv, cellv, wt, last_ref, fin_ref,
               dg_hbm, tlo_hbm, tlf_hbm, bias_ref, hfin_ref, cfin_ref,
               wupt, dout, gyv, dgv, dgr, dgch, dgs, dct, bacc, own, snd, rcv, pin, pout, bsnd, brcv, finr,
               lsem, osem, xs, xr, gs, grs, ps, prs, csem, bsem, tsem):
    y, m, x, c = place()
    beside, across, skew = flips(m)
    nch = dgv.shape[_0]
    half = dct.shape[_1]
    hl = half // _2
    wide = 4 * hl
    hp = PAIRS // _2
    hr = ROWS // _2

    up_loads = [local(wupt_hbm.at[:, aligned(shard, hl)], wupt.at[:, pl.ds(pos * hl, hl)], lsem.at[pos])
                for pos, shard in enumerate((_1 - c, 3 - c, c, _2 + c))]

    @pl.when(x == _1)
    def _():
        local(gy_hbm, gyv, lsem.at[4]).start()
    for cp in up_loads:
        cp.start()
    entry_barrier(y, m)

    own_cols = pl.ds(pl.multiple_of(c * half, half), half)

    def last_sends():
        return [remote(last_ref, (tlo_hbm if i < 3 else tlf_hbm).at[:, own_cols], tsem.at[i],
                       tsem.at[9] if i < 3 else tsem.at[10], dev(oy, om))
                for i, (oy, om) in enumerate(everyone(y, m))]

    def last_keep():
        return local(last_ref, tlo_hbm.at[:, own_cols], tsem.at[11])

    def fin_send():
        return remote(fin_ref.at[_1], finr, tsem.at[7], tsem.at[8], dev(y, across))

    @pl.when(x == _1)
    def _():
        for cp in last_sends():
            cp.start()
        last_keep().start()
    fin_send().start()

    def swap(slot):
        return remote(snd.at[slot], rcv.at[slot], xs.at[slot], xr.at[slot], dev(y, beside))

    part_a = pl.ds(_0, wide)
    part_b = pl.ds(wide, wide)

    def half_rows(k, h):
        return pl.ds(pl.multiple_of(k * ROWS, ROWS) + h * hr, hr)

    def up_grads(k, h):
        rows = pl.ds(h * hr, hr)
        return remote(dgv.at[k, rows, part_b], dgr.at[k, rows], gs.at[_0, h], grs.at[k, h], dev(y, across))

    def near(k, h, top):
        if top:
            return up_grads(k, h)
        return remote(dgv.at[k, pl.ds(h * hr, hr), part_b], dg_hbm.at[_0, _0, half_rows(k, h), :],
                      gs.at[_0, h], csem.at[_2], dev(y, across))

    def wider(k, h, i):
        rows = pl.ds(pl.multiple_of(h * hr, hr), hr)
        dst = dg_hbm.at[x, _1, pl.ds(pl.multiple_of(k * ROWS + h * hr, hr), hr), :]
        src, other = ((part_a, m), (part_b, across))[i]
        return remote(dgv.at[k, rows, src], dst, gs.at[_1 + i, h], csem.at[i], dev(_1 - y, other))

    def keep(k, h, top):
        return local(dgv.at[k, pl.ds(h * hr, hr), part_a], dg_hbm.at[_1 if top else _0, _0, half_rows(k, h), :], osem.at[_0])

    def keep_up(k):
        return local(dgr.at[k], dg_hbm.at[_1, _0, aligned(k, ROWS), :], osem.at[_1])

    def psend(k, pos, piece, dest, src):
        rows = pl.ds(piece * hp, hp)
        return remote(pout.at[pos, rows], pin.at[src, k, rows], ps.at[pos, piece], prs.at[src, k, piece], dev(y, dest))

    def up_sends(k, pos):
        return [psend(k, pos, piece, skew if pos == _0 else across, c) for piece in (_1, _0)]

    def side_sends(k):
        return [psend(k, _0, piece, beside, _2) for piece in (_1, _0)]

    dct[...] = jnp.zeros(dct.shape, F32)
    bacc[...] = jnp.zeros(bacc.shape, F32)

    @pl.when(x == _1)
    def _():
        local(gy_hbm, gyv, lsem.at[4]).wait()
        for s in BOTH:
            dout[:, :, part(s, hl)] = gyv[s].astype(F32).reshape(nch * PAIRS, 8, hl)

    @pl.when(x == _0)
    def _():
        for cp in up_loads:
            cp.wait()

    def point(k, p, j, inner):
        pair = k * PAIRS + p
        rows = part(j, BATCH)
        for s in BOTH:
            base = s * wide
            units = part(s, hl)
            gi, gf, go, gu = (actv[pair, rows, part(g, hl, base)] for g in GATES)
            tc = jnp.tanh(cellv[pair + _1, rows, units])
            cp = cellv[pair + _1, _0:4, units] if j else cellv[pair, 4:8, units]
            dh = dout[pair, rows, units]
            if inner:
                dh = dh + own[:, units] + rcv[j, :, units]
            dc = dct[:, units] + dh * go * (1.0 - tc * tc)
            dct[:, units] = dc * gf
            grads = (dc * gu * gi * (1.0 - gi), dc * cp * gf * (1.0 - gf),
                     dh * tc * go * (1.0 - go), dc * gi * (1.0 - gu * gu))
            for g, val in enumerate(grads):
                cols = part(g, hl, base)
                dgs[:, cols] = val.astype(BF16)
                dgch[p, rows, cols] = val

    def step(k, p, j, after):
        dgl = dgs[...]
        snd[j] = mm(dgl, wt[:, _0:half])
        swap(j).start()
        own[...] = mm(dgl, wt[:, half:])
        swap(j).wait()
        after()
        point(k, p, j, True)

    def again(make, k):
        @pl.when(k < nch - _1)
        def _():
            make(k + _1).wait_send()
        make(k).start()

    def near_copy(h, top):
        return lambda k: near(k, h, top)

    def first_turn(k, e):
        late = k < nch - _1

        if e == _0:
            @pl.when((x == _0) & late)
            def _():
                again(near_copy(_0, False), k + _1)

        @pl.when((x == _1) & late)
        def _():
            up_sends(k + _1, e)[_1].start()

    def turn(k, p, j):
        back = p - _1
        q = k + back

        @pl.when((p >= _1) & (q < nch))
        def _():
            again(lambda v: wider(v, _1 - back, _1 - j), q)

        if j == _1:
            @pl.when((p == _0) & (x == _0))
            def _():
                again(near_copy(_1, False), k)

    def emit(k, h):
        dgv[k, part(h, hr), :] = dgch[part(h, hp)].reshape(hr, _2 * wide).astype(BF16)
        total = dgch[h * hp]
        for p in range(h * hp + _1, (h + _1) * hp):
            total = total + dgch[p]
        bacc[...] += total

        @pl.when(x == _0)
        def _():
            keep(k, h, False).start()

        @pl.when(x == _1)
        def _():
            again(near_copy(h, True), k)
            keep(k, h, True).start()

    def take(k, piece):
        for src in (_0, _1, _2):
            psend(k, _0, piece, beside, src).wait_recv()
        rows = pl.ds(piece * hp, hp)
        dout[pl.ds(k * PAIRS + piece * hp, hp)] = pout[_1, rows] + pin[_0, k, rows] + pin[_1, k, rows] + pin[_2, k, rows]

    def slot_body(s, _):
        k = nch - _1 - s + (_1 - x)
        live = (k >= _0) & (k < nch)
        first = live & (k == nch - _1)

        @pl.when((x == _0) & live)
        def _():
            @pl.when(k < nch - _1)
            def _():
                for cp in side_sends(k + _1):
                    cp.wait_send()
            up_grads(k, _1).wait_recv()
            up_grads(k, _0).wait_recv()
            keep_up(k).start()
            block = dgr[k]
            pout[_0] = mm(block, wupt[:, _0:half]).reshape(PAIRS, 8, half)
            for cp in side_sends(k):
                cp.start()
            pout[_1] = mm(block, wupt[:, half:]).reshape(PAIRS, 8, half)
            take(k, _1)

        @pl.when(live)
        def _():
            @pl.when(first)
            def _():
                point(k, PAIRS - _1, _1, False)

                @pl.when(x == _1)
                def _():
                    for cp in up_loads:
                        cp.wait()

            @pl.when(k < nch - _1)
            def _():
                step(k, PAIRS - _1, _1, lambda: first_turn(k, _0))
            step(k, PAIRS - _1, _0, lambda: first_turn(k, _1))

            def pair_body(i, _):
                p = PAIRS - _2 - i

                @pl.when((x == _0) & (p == hp - _1))
                def _():
                    take(k, _0)

                step(k, p, _1, lambda: turn(k, p, _1))
                step(k, p, _0, lambda: turn(k, p, _0))

                @pl.when(p == hp)
                def _():
                    emit(k, _1)
                return _0

            lax.fori_loop(_0, PAIRS - _1, pair_body, _0)
            emit(k, _0)

        @pl.when((x == _1) & live)
        def _():
            @pl.when(k < nch - _1)
            def _():
                for pos in BOTH:
                    for cp in up_sends(k + _1, pos):
                        cp.wait_send()
            block = dgv[k, :, _0:wide]
            for pos in BOTH:
                pout[pos] = mm(block, wupt[:, part(pos, half)]).reshape(PAIRS, 8, half)
                up_sends(k, pos)[_0].start()
        return _0

    lax.fori_loop(_0, nch + _1, slot_body, _0)

    @pl.when(x == _0)
    def _():
        again(near_copy(_0, False), _0)

    @pl.when(x == _1)
    def _():
        for pos in BOTH:
            up_sends(_0, pos)[_1].start()
    for i in BOTH:
        again(lambda v: wider(v, _0, i), _0)

    bsnd[_0] = bacc[:, _0:wide]
    bsnd[_1] = bacc[:, wide:]
    shares = (remote(bsnd.at[_0], brcv.at[_0], bsem.at[_0], bsem.at[3], dev(_1 - y, m)),
              remote(bsnd.at[_1], brcv.at[_1], bsem.at[_1], bsem.at[4], dev(y, across)),
              remote(bsnd.at[_1], brcv.at[_2], bsem.at[_2], bsem.at[5], dev(_1 - y, across)))
    for cp in shares:
        cp.start()

    fin_send().wait()
    for ref, i in ((hfin_ref, _0), (cfin_ref, _1)):
        ref[_0] = jnp.where(x == _0, fin_ref[_0, i], finr[i])
        ref[_1] = jnp.where(x == _0, finr[i], fin_ref[_0, i])

    quarter = dg_hbm.at[_0, _0]

    @pl.when(x == _0)
    def _():
        for cp in side_sends(_0):
            cp.wait_send()
        for h in BOTH:
            near(_0, h, False).wait_send()
        local(quarter, quarter, osem.at[_1]).wait()
        local(tlo_hbm, tlo_hbm, tsem.at[9]).wait()

    @pl.when(x == _1)
    def _():
        for pos in BOTH:
            for cp in up_sends(_0, pos):
                cp.wait_send()
        for h in BOTH:
            near(_0, h, True).wait_send()
        local(quarter, quarter, csem.at[_2]).wait()
        for cp in last_sends():
            cp.wait_send()
        local(last_ref, last_ref, tsem.at[9]).wait()
        last_keep().wait()

    for h in BOTH:
        for i in BOTH:
            wider(_0, h, i).wait_send()
    local(tlf_hbm, tlf_hbm, tsem.at[10]).wait()
    local(quarter, quarter, csem.at[_0]).wait()
    local(quarter, quarter, csem.at[_1]).wait()
    local(quarter, quarter, osem.at[_0]).wait()
    for cp in shares:
        cp.wait()
    same = jnp.sum(bsnd[_0] + brcv[_0], axis=_0, keepdims=True)
    cross = jnp.sum(brcv[_1] + brcv[_2], axis=_0, keepdims=True)
    low = jnp.where(x == _0, same, cross)
    top = jnp.where(x == _0, cross, same)
    for g in GATES:
        bias_ref[_0, g:g + _1, :] = low[:, part(g, hl)]
        bias_ref[_1, g:g + _1, :] = top[:, part(g, hl)]


def grad_kernel(xo_hbm, xf_hbm, lo_hbm, to_hbm, far_hbm, tlo_hbm, tlf_hbm, init_ref, hs_ref, cs_ref, bs_ref, dg_hbm,
                dwin_hbm, dwup_hbm, dwrec_hbm, y_ref, hfin_ref, cfin_ref, bias_ref,
                lhs, grads, htop, shf, yf, lhst0, lhst1, pieces0, pieces1, lsem, osem):
    hidden = htop.shape[_1]
    srows = lo_hbm.shape[_0]
    lhst = (lhst0, lhst1)
    pieces = (pieces0, pieces1)
    kb = lhst0.shape[_0]
    hl = hidden // 4
    nblk = hidden // kb
    per = hl // LANES
    nq = hl // kb
    m = lax.axis_index('model')
    x = m // _2
    c = m % _2
    lo = pl.ds(_0, srows)
    hi = pl.ds(srows, srows)
    body_rows = pl.ds(_0, srows - ROWS)
    srcs = ((xo_hbm, lhs.at[_0, lo, :]), (xf_hbm, lhs.at[_0, hi, :]), (dg_hbm.at[_0, _0], grads.at[_0, lo, :]), (dg_hbm.at[_0, _1], grads.at[_0, hi, :]),
            (lo_hbm, lhs.at[_1, lo, :]), (far_hbm.at[_0], lhs.at[_1, hi, :]), (dg_hbm.at[_1, _0], grads.at[_1, lo, :]), (dg_hbm.at[_1, _1], grads.at[_1, hi, :]),
            (to_hbm.at[body_rows, :], htop.at[body_rows, :]),
            (far_hbm.at[_1, body_rows, :], htop.at[pl.ds(srows, srows - ROWS), :]),
            (tlo_hbm, htop.at[pl.ds(srows - ROWS, ROWS), :]), (tlf_hbm, htop.at[pl.ds(_2 * srows - ROWS, ROWS), :]))
    loads = [local(a, b, lsem.at[i]) for i, (a, b) in enumerate(srcs)]
    for cp in loads:
        cp.start()

    def core_row(i):
        q = i // nq
        return ((q % _2) * _2 + q // _2) * nq + i % nq

    def out_start(slot, n):
        ph = n // nblk
        i = lax.rem(n, nblk)

        def put(dst, off):
            for j in range(4 * per):
                local(pieces[slot].at[j], dst.at[aligned(off, kb), j, :], osem.at[slot]).start()

        @pl.when(ph == _0)
        def _():
            put(dwin_hbm, i)

        @pl.when(ph == _1)
        def _():
            put(dwup_hbm, core_row(i))

        @pl.when(ph >= _2)
        def _():
            put(dwrec_hbm, (ph - _2) * nblk + core_row(i))

    def out_wait(slot):
        local(pieces[slot], pieces[slot], osem.at[slot]).wait()

    def shift(src, dst, layer, i):
        cols = aligned(i, kb)
        for part in BOTH:
            base = part * srows
            shf[base + 4:base + srows, :] = src[pl.ds(base, srows), cols].astype(F32)[:srows - 4]
            shf[base:base + 4, :] = init_ref[layer, part, :, cols].astype(F32)
        dst[:, cols] = shf[...].astype(BF16)

    def prepare(slot, n):
        lhst[slot][...] = lhs[n // nblk, :, aligned(lax.rem(n, nblk), kb)].T

    total = 4 * nblk
    for ref, dst in ((hs_ref, hfin_ref), (cs_ref, cfin_ref), (bs_ref, bias_ref)):
        dst[...] = ref[...]
    for cp in loads[_0:4]:
        cp.wait()
    prepare(_0, _0)

    def body(it, _):
        @pl.when(it == nblk // _2 - _1)
        def _():
            for cp in loads[4:]:
                cp.wait()

        @pl.when((it >= nblk // _2) & (it < nblk))
        def _():
            for e in BOTH:
                i = _2 * it + e - nblk
                shift(lhs.at[_1], lhs.at[_2], _0, i)
                shift(htop, lhs.at[3], _1, i)

        for e in BOTH:
            n = _2 * it + e

            @pl.when(n >= _2)
            def _():
                out_wait(e)
            res = mm(lhst[e][...], grads[lax.rem(n // nblk, _2)])
            for g in GATES:
                for ct in range(per):
                    col = g * hl + ct * LANES
                    pieces[e][ct * 4 + g] = res[:, col:col + LANES]
            prepare(_1 - e, jnp.minimum(n + _1, total - _1))
            out_start(e, n)
        return _0

    lax.fori_loop(_0, total // _2, body, _0)
    for t in range(per):
        yf[t] = htop[_0:srows, pl.ds(pl.multiple_of(c * _2 * hl + x * hl + t * LANES, LANES), LANES)].astype(F32)
        for b in range(BATCH):
            y_ref[b, :, part(t, LANES)] = yf[t, pl.ds(b, srows // BATCH, stride=BATCH), :].astype(BF16)
    for slot in BOTH:
        out_wait(slot)


def any_spec():
    return pl.BlockSpec(memory_space=pl.ANY)


def vmem_spec():
    return pl.BlockSpec(memory_space=pltpu.VMEM)


def sds(shape, dtype):
    return jax.ShapeDtypeStruct(shape, dtype)


DMA = pltpu.SemaphoreType.DMA


def comm_params(i, limit=VMEM_LIMIT):
    return pltpu.CompilerParams(collective_id=i, has_side_effects=True, vmem_limit_bytes=limit)


def run_prep(wrec, wup, win, x, gy, h, c, bias):
    batch, seq, width = x.shape
    hl = gy.shape[_2]
    wide = 4 * hl
    hidden = 4 * hl
    rows = batch * seq
    raw = win.shape[_0]
    per = hl // LANES
    span = KB * 4 * per
    square = sds((hidden, wide), BF16)
    vm = pltpu.VMEM
    return pl.pallas_call(
        prep_kernel,
        name='lstm_prepare',
        out_shape=(square,) * 6 + (sds((rows // 8, 8, wide), F32), sds((rows, width), BF16), sds((_2, rows, hl), BF16),
                                   sds((_2, 4, hl), F32), sds((_2, _2, 4, hidden), BF16)),
        in_specs=[any_spec()] * 5 + [vmem_spec()] * 3,
        out_specs=(any_spec(),) * 9 + (vmem_spec(),) * _2,
        scratch_shapes=[
            vm((raw, LANES), BF16), vm((raw, LANES), BF16), vm((raw, LANES), BF16), vm((raw, LANES), BF16),
            vm((_2, span, LANES), F32), vm((6, KB, wide), BF16), vm((6, wide, KB), BF16), vm((width, wide), BF16),
            vm(x.shape, BF16), vm((4, rows, LANES), F32), vm((rows, width), BF16), vm((rows // 8, 8, wide), F32),
            vm(gy.shape, BF16), vm((rows, hl), BF16), vm((_2, 4, hl), BF16),
            vm((_2, _2, 4, hidden), BF16), vm((_2, 4, hl), F32),
            DMA((5,)), DMA((3,)), DMA((6, _2)), DMA((NX,)), DMA((NX,)), DMA((NX,)), DMA((NX,)), DMA((9,)), DMA((9,)), DMA((_2,)),
        ],
        compiler_params=comm_params(_0),
    )(wrec, wup, win, x, gy, h, c, bias)


def run_fwd(wa, wb, wup, pre, xt, wta, wtb, h, c, hcb, bias):
    hidden, wide = wa.shape
    hl = wide // 4
    half = _2 * hl
    npair = pre.shape[_0]
    nch = npair // PAIRS
    rows = npair * 8
    hist = sds((rows, hidden), BF16)
    vm = pltpu.VMEM
    return pl.pallas_call(
        fwd_kernel,
        name='lstm_forward',
        out_shape=(vm((npair, 8, _2 * wide), F32), vm((npair + _1, 8, half), F32), vm((_2 * wide, hidden), BF16),
                   hist, hist, sds((_2, rows, hidden), BF16),
                   sds(xt.shape, BF16), sds((ROWS, half), BF16), sds((_2, _2, 4, hl), F32)),
        in_specs=[any_spec()] * 7 + [vmem_spec()] * 4,
        out_specs=(vmem_spec(),) * 3 + (any_spec(),) * 4 + (vmem_spec(),) * _2,
        scratch_shapes=[
            vm((hidden, _2 * wide), BF16), vm((hidden, wide), BF16),
            vm((npair + PAIRS, 8, wide), F32), vm((npair, 8, wide), F32),
            vm((nch, ROWS, half), BF16), vm((nch, ROWS, hidden), BF16),
            vm((PAIRS, 8, half), F32), vm((4, half), F32),
            vm((_2, _2, 4, hl), BF16), vm((_2, _2, 4, hl), BF16),
            DMA((12,)), DMA((nch,)), DMA((4,)), DMA((_2, _2)), DMA((_2, _2)), DMA((7,)), DMA((nch, _2)),
            DMA((PAIRS,)), DMA((npair,)), DMA((3,)), DMA((3,)),
        ],
        compiler_params=comm_params(_1, STEP_LIMIT),
    )(wa, wb, wup, pre, xt, wta, wtb, h, c, hcb, bias)


def run_bwd(wupt, gy, act, cell, wt, last, fin):
    wide, hidden = wupt.shape
    hl = wide // 4
    half = _2 * hl
    npair = act.shape[_0]
    nch = npair // PAIRS
    rows = npair * 8
    vm = pltpu.VMEM
    state = sds((_2, 4, hl), F32)
    return pl.pallas_call(
        bwd_kernel,
        name='lstm_backward',
        out_shape=(sds((_2, _2, rows, wide), BF16), sds((ROWS, hidden), BF16), sds((ROWS, hidden), BF16), state, state, state),
        in_specs=[any_spec()] * _2 + [vmem_spec()] * 5,
        out_specs=(any_spec(),) * 3 + (vmem_spec(),) * 3,
        scratch_shapes=[
            vm((wide, hidden), BF16), vm((npair, 8, half), F32), vm((_2, rows, hl), BF16),
            vm((nch, ROWS, _2 * wide), BF16), vm((nch, ROWS, wide), BF16),
            vm((PAIRS, 8, _2 * wide), F32), vm((4, _2 * wide), BF16),
            vm((4, half), F32), vm((8, _2 * wide), F32),
            vm((4, half), F32), vm((_2, 4, half), F32), vm((_2, 4, half), F32),
            vm((3, nch, PAIRS, 8, half), F32), vm((_2, PAIRS, 8, half), F32),
            vm((_2, 8, wide), F32), vm((3, 8, wide), F32), vm((_2, 4, hl), F32),
            DMA((5,)), DMA((_2,)), DMA((_2,)), DMA((_2,)), DMA((3, _2)), DMA((nch, _2)), DMA((_2, _2)), DMA((3, nch, _2)),
            DMA((3,)), DMA((6,)), DMA((12,)),
        ],
        compiler_params=comm_params(_2, STEP_LIMIT),
    )(wupt, gy, act, cell, wt, last, fin)


def run_grads(xo, xf, lo, to, far, tlo, tlf, init, small, dg):
    srows, hidden = lo.shape
    rows = _2 * srows
    wide = dg.shape[3]
    tile = (wide // LANES, LANES)
    hl = wide // 4
    kb = 512
    vm = pltpu.VMEM
    return pl.pallas_call(
        grad_kernel,
        name='weight_grads',
        out_shape=(sds((hidden,) + tile, F32), sds((hidden,) + tile, F32), sds((_2 * hidden,) + tile, F32),
                   sds((BATCH, srows // BATCH, hl), BF16)) + (sds((_2, 4, hl), F32),) * 3,
        in_specs=[any_spec()] * 7 + [vmem_spec()] * 4 + [any_spec()],
        out_specs=(any_spec(),) * 3 + (vmem_spec(),) * 4,
        scratch_shapes=[vm((4, rows, hidden), BF16), vm((_2, rows, wide), BF16), vm((rows, hidden), BF16),
                        vm((rows, kb), F32), vm((hl // LANES, srows, LANES), F32), vm((kb, rows), BF16), vm((kb, rows), BF16),
                        vm((wide // LANES, kb, LANES), F32), vm((wide // LANES, kb, LANES), F32), DMA((12,)), DMA((_2,))],
        compiler_params=pltpu.CompilerParams(vmem_limit_bytes=VMEM_LIMIT),
    )(xo, xf, lo, to, far, tlo, tlf, init, *small, dg)


def to_raw(w):
    hl = w.shape[-_1]
    w = w.reshape(-_1, 4, hl // LANES, LANES)
    return jnp.swapaxes(w, _1, _2).reshape(-_1, LANES)


def from_raw(v, lead, hl):
    v = v.reshape(-_1, hl // LANES, 4, LANES)
    return jnp.swapaxes(v, _1, _2).reshape(lead + (-_1, 4, hl))


def solution(mesh):
    batch_axes = ('part', 'data')
    seq_spec = P(batch_axes, None, 'model')
    state_spec = P(None, batch_axes, 'model')
    weight_spec = P(None, None, None, 'model')
    in_specs = (P(batch_axes, None, None), seq_spec, state_spec, state_spec,
                P(None, None, 'model'), weight_spec, weight_spec, P(None, None, 'model'))
    out_specs = (seq_spec, state_spec, state_spec, P('part', None, 'model'),
                 P(None, 'part', None, 'model'), P(None, 'part', None, 'model'), P(None, 'part', 'model'))

    def local_program(x_seq, gy_seq, h_init, c_init, w_in, w_up, w_rec, gate_bias):
        hl = w_in.shape[_2]
        wa, wb, wat, wbt, wup, wupt, pre, xt, gyt, hcb, init = run_prep(
            to_raw(w_rec), to_raw(w_up), to_raw(w_in), x_seq, gy_seq, h_init, c_init, gate_bias)
        act, cell, wt, low_own, top_own, far, x_far, last, fin = run_fwd(
            wa, wb, wup, pre, xt, wat, wbt, h_init, c_init, hcb, gate_bias)
        act, cell, wt = (pltpu.with_memory_space_constraint(v, pltpu.VMEM) for v in (act, cell, wt))
        dg, last_own, last_far, bias, h_last, c_last = run_bwd(wupt, gyt, act, cell, wt, last, fin)
        dw_in, dw_up, dw_rec, y_out, h_last, c_last, bias = run_grads(
            xt, x_far, low_own, top_own, far, last_own, last_far, init, (h_last, c_last, bias), dg)
        return (y_out, h_last, c_last, from_raw(dw_in, (), hl), from_raw(dw_up, (_1,), hl),
                from_raw(dw_rec, (_2,), hl), bias)

    return jax.shard_map(local_program, mesh=mesh, in_specs=in_specs, out_specs=out_specs, check_vma=False)
```
